256 devices in a mesh: node: 8 (over z_lo, core), local: 32 (over y, x, z_hi).
Axes of the slice: x: 4, y: 4, z: 8 (z_hi: 2, z_lo: 4; z = z_hi * 4 + z_lo), core: 2. Of those that a mesh axis runs over, the one named last changes fastest.
Arguments:
- partials: bfloat16 [8, 32, 1048576], P('node', 'local'), may hold values from -8 to 8
- signs: int32 [1048576], replicated, may hold values 0 or 1
Outputs:
- reduced: float32 [1048576], P(('node', 'local'))
- rotated_max: float32 [8192], P(('node', 'local'))
The draws below stay inside these ranges and needn't reach their ends.
Inputs may be any that keep to these rules, and one draw needn't show every extreme that they name: `signs`: 0 selects the sign +1 and 1 the sign -1 of a position.
All inputs are finite; a program needn't handle non-finite values.
Results may differ from the reference program's by a relative error of at most 0.0003.
Values may be sent and summed in bfloat16 or wider, within the bound.
A program may use at most 64 MiB of HBM per device.

```python
import math
import jax
import jax.numpy as jnp
from jax import lax

BUCKET = 1048576
ROT = 256
QGROUP = 128
GROUPS = 8
MEMBERS = 32


def draw_partials(key, part):
    streams = jax.random.split(jax.random.fold_in(key, 7001), 2)
    shape = (GROUPS, MEMBERS, BUCKET)
    noise = jax.random.normal(streams[0], shape, jnp.float32)
    replica_scale = jnp.exp(jax.random.uniform(streams[1], (GROUPS, MEMBERS, 1), jnp.float32, math.log(0.8), math.log(1.2)))
    magnitude = jnp.clip(jnp.abs(noise), 1.0 / 16.0, 4.0)
    direction = jnp.where(noise >= 0.0, 1.0, -1.0)
    values = direction * magnitude * replica_scale / 16.0
    return values.astype(jnp.bfloat16)


def touch_ends(values, rng, least, high):
    place = [jax.random.randint(jax.random.fold_in(rng, axis), (), 0, length) for axis, length in enumerate(values.shape)]
    widest = values.shape.index(max(values.shape))
    next_to = place[:widest] + [(place[widest] + 1) % values.shape[widest]] + place[widest + 1:]
    return values.at[tuple(place)].set(least).at[tuple(next_to)].set(high)


def setup_inputs(seed: int = 0) -> dict:
    key_of = jax.random.split(jax.random.key(seed), 3)
    partials = draw_partials(jax.random.fold_in(key_of[2], 71), 0)
    signs = touch_ends((jax.random.randint(key_of[1], (BUCKET,), 0, 2) < 1).astype(jnp.int32), jax.random.fold_in(key_of[1], 1), 0, 1)
    return {"partials": partials, "signs": signs}


def sylvester():
    positions = jnp.arange(ROT, dtype=jnp.int32)
    parity = jnp.zeros((ROT, ROT), dtype=jnp.int32)
    for level in range(ROT.bit_length() - 1):
        column = positions >> level & 1
        parity = parity + column[:, None] * column[None, :]
    return (1 - 2 * (parity % 2)).astype(jnp.float32)

def power_scale(largest):
    scaling = jnp.full(largest.shape, 2.0 ** (-37), dtype=jnp.float32)
    for power in range(-30, 31):
        scaling = jnp.where(largest >= 2.0 ** power, jnp.float32(2.0 ** (power - 7)), scaling)
    return scaling

def quantize(scaled):
    magnitude = jnp.abs(scaled)
    spacing = jnp.full(scaled.shape, 2.0 ** (-9), dtype=jnp.float32)
    for power in range(-5, 8):
        spacing = jnp.where(magnitude >= 2.0 ** power, jnp.float32(2.0 ** (power - 3)), spacing)
    return jnp.sign(scaled) * jnp.floor(magnitude / spacing + 0.5) * spacing

def encode(values):
    grouped = values.reshape(values.shape[:-1] + (values.shape[-1] // QGROUP, QGROUP))
    largest = lax.optimization_barrier(jnp.max(jnp.abs(grouped), axis=-1))
    scaling = power_scale(largest)
    coded = quantize(grouped / scaling[..., None]).astype(jnp.bfloat16)
    return (coded.reshape(values.shape), scaling.astype(jnp.bfloat16))

def decode(coded, scales):
    grouped = coded.reshape(coded.shape[:-1] + (coded.shape[-1] // QGROUP, QGROUP))
    values = grouped.astype(jnp.float32) * scales.astype(jnp.float32)[..., None]
    return values.reshape(coded.shape)

def reference(partials, signs):
    flips = (1 - 2 * signs).astype(jnp.float32)
    matrix = sylvester()

    def group_sum(replicas):
        signed = replicas.astype(jnp.float32) * flips
        rotated = jnp.dot(signed.reshape(-1, ROT), matrix, precision=lax.Precision.HIGHEST, preferred_element_type=jnp.float32).reshape(signed.shape)
        coded, scales = encode(rotated)
        first = lax.optimization_barrier(jnp.sum(decode(coded, scales), axis=0))
        coded_two, scales_two = encode(first)
        return decode(coded_two, scales_two)
    group_parts = lax.map(group_sum, partials)
    second = lax.optimization_barrier(jnp.sum(group_parts, axis=0))
    rotated_max = lax.optimization_barrier(jnp.max(jnp.abs(second.reshape(-1, QGROUP)), axis=-1)) / jnp.sqrt(jnp.float32(ROT))
    turned_back = jnp.dot(second.reshape(-1, ROT), matrix, precision=lax.Precision.HIGHEST, preferred_element_type=jnp.float32).reshape(second.shape)
    reduced = turned_back / ROT * flips
    return (reduced, rotated_max)
```

```python
import functools

import jax
import jax.numpy as jnp
from jax import lax
from jax.experimental import pallas as pl
from jax.experimental.pallas import tpu as pltpu
from jax.sharding import PartitionSpec as P

ROT = 256
QGROUP = 128
MESH = pl.DeviceIdType.MESH
NEAR_LAST = (2, 1, 3, 0)


def power_below(values):
    lifted = values * 2.0**23
    nearest = (values + lifted) - lifted
    return jnp.where(nearest > values, 0.5 * nearest, nearest)


def encode(values):
    largest = jnp.max(jnp.abs(values), axis=0, keepdims=True)
    power = power_below(jnp.clip(largest, 2.0**-30, 1.5 * 2.0**30))
    inverse = 1.0 / power
    lifted = inverse * 2.0**23
    inverse = (inverse + lifted) - lifted
    units = jnp.trunc(values * (inverse * 2.0**17))
    anchor = jnp.maximum(jnp.abs(units) * 2.0**20, 1.5 * 2.0**24)
    code = (units * (1.0 + 2.0**-20) + anchor) - anchor
    return code * (power * 2.0**-17)


def kernel(
    x_hbm,
    signs_hbm,
    out_ref,
    max_ref,
    x_in,
    signs_in,
    own_signs,
    matrix,
    rows,
    coded,
    got_a,
    part,
    got_b,
    pair,
    got_c,
    recoded,
    got_n,
    in_sem,
    a_send,
    a_recv,
    b_send,
    b_recv,
    c_send,
    c_recv,
    n_send,
    n_recv,
):
    node, local = lax.axis_index("node"), lax.axis_index("local")
    me_y, me_x, me_z = local // 8, lax.rem(local // 2, 4), lax.rem(local, 2)

    def ahead(place, step):
        return lax.rem(place + step, 4)

    def device(y, x, z):
        return (node, y * 8 + x * 2 + z)

    def place_z(own):
        return me_z if own else 1 - me_z

    first_of = (me_x, me_y)
    second_of = (me_y, me_x)

    def along_first(h, step):
        if h == 0:
            return device(me_y, ahead(me_x, step), me_z)
        return device(ahead(me_y, step), me_x, me_z)

    def along_second(h, step):
        return along_first(1 - h, step)

    barrier = pltpu.get_barrier_semaphore()
    for h in range(2):
        for step in range(1, 4):
            pl.semaphore_signal(barrier, inc=1, device_id=along_first(h, step), device_id_type=MESH)
    pl.semaphore_signal(barrier, inc=1, device_id=device(me_y, me_x, 1 - me_z), device_id_type=MESH)
    for step in range(1, 8):
        pl.semaphore_signal(
            barrier, inc=1, device_id=(lax.rem(node + step, 8), local), device_id_type=MESH
        )

    def tile_of(own, dy, dx):
        return ahead(me_y, dy) * 8 + ahead(me_x, dx) * 2 + place_z(own)

    def load(own, dy, dx):
        t = tile_of(own, dy, dx)
        return (
            pltpu.make_async_copy(x_hbm.at[:, t], x_in.at[t], in_sem.at[0, t]),
            pltpu.make_async_copy(signs_hbm.at[:, t], signs_in.at[t], in_sem.at[1, t]),
        )

    for own in range(2):
        for dy in NEAR_LAST:
            for dx in NEAR_LAST:
                for copy in load(own, dy, dx):
                    copy.start()
    own_copy = pltpu.make_async_copy(signs_hbm.at[node, local], own_signs, in_sem.at[0, 32])
    own_copy.start()

    i = lax.broadcasted_iota(jnp.int32, (ROT, ROT), 0)
    j = lax.broadcasted_iota(jnp.int32, (ROT, ROT), 1)
    odd = lax.population_count(i & j) & 1
    matrix[...] = (1 - 2 * odd).astype(jnp.float32).astype(jnp.bfloat16)

    def send_a(own, h, c, step):
        return pltpu.make_async_remote_copy(
            src_ref=coded.at[h, own, c, ahead(first_of[h], step)],
            dst_ref=got_a.at[h, own, c, step - 1],
            send_sem=a_send.at[h, own, c, step - 1],
            recv_sem=a_recv.at[h, own, c, step - 1],
            device_id=along_first(h, step),
            device_id_type=MESH,
        )

    def send_b(own, h, step):
        return pltpu.make_async_remote_copy(
            src_ref=part.at[h, own, ahead(second_of[h], step)],
            dst_ref=got_b.at[h, own, step - 1],
            send_sem=b_send.at[h, own, step - 1],
            recv_sem=b_recv.at[h, own, step - 1],
            device_id=along_second(h, step),
            device_id_type=MESH,
        )

    def send_c(h):
        return pltpu.make_async_remote_copy(
            src_ref=pair.at[h],
            dst_ref=got_c.at[h],
            send_sem=c_send.at[h],
            recv_sem=c_recv.at[h],
            device_id=device(me_y, me_x, 1 - me_z),
            device_id_type=MESH,
        )

    def send_n(step):
        to = lax.rem(node + step, 8)
        return pltpu.make_async_remote_copy(
            src_ref=recoded.at[to],
            dst_ref=got_n.at[step - 1],
            send_sem=n_send.at[step - 1],
            recv_sem=n_recv.at[step - 1],
            device_id=(to, local),
            device_id_type=MESH,
        )

    def rotate_row(own, dy):
        for dx in NEAR_LAST:
            for copy in load(own, dy, dx):
                copy.wait()
        for k, dx in enumerate(NEAR_LAST):
            t = tile_of(own, dy, dx)
            for g in range(8):
                for q in range(4):
                    v = x_in[t, g, :, pl.ds(q * 1024, 1024)].astype(jnp.float32).reshape(8, 128)
                    s = signs_in[t, g, pl.ds(q * 8, 8), :]
                    rows[k, pl.ds(g * 32 + q * 8, 8), :] = jnp.where(s == 0, v, -v)
        for k, dx in enumerate(NEAR_LAST):
            blocks = jnp.concatenate(
                [
                    rows[k, pl.ds(0, 128, 2), :].astype(jnp.bfloat16),
                    rows[k, pl.ds(1, 128, 2), :].astype(jnp.bfloat16),
                ],
                axis=1,
            )
            rotated = lax.dot_general(
                matrix[...],
                blocks,
                (((1,), (1,)), ((), ())),
                preferred_element_type=jnp.float32,
            )
            y, x = ahead(me_y, dy), ahead(me_x, dx)
            coded[0, own, y, x] = encode(rotated[:QGROUP]).astype(jnp.bfloat16)
            coded[1, own, x, y] = encode(rotated[QGROUP:]).astype(jnp.bfloat16)

    def send_row(own, dy):
        y = ahead(me_y, dy)
        for dx in NEAR_LAST[:3]:
            send_a(own, 0, y, dx).start()
        if dy:
            for dx in NEAR_LAST:
                send_a(own, 1, ahead(me_x, dx), dy).start()

    def add_first(own, h, c):
        for step in range(1, 4):
            send_a(own, h, c, step).wait_recv()
        total = coded[h, own, c, first_of[h]].astype(jnp.float32)
        for step in range(1, 4):
            total += got_a[h, own, c, step - 1].astype(jnp.float32)
        return total

    def reduce_first(own, step):
        for h in range(2):
            c = ahead(second_of[h], step)
            part[h, own, c] = add_first(own, h, c)
            if step:
                send_b(own, h, step).start()

    def reduce_second(own, h):
        for step in range(1, 4):
            send_b(own, h, step).wait_recv()
        total = part[h, own, second_of[h]]
        for step in range(1, 4):
            total += got_b[h, own, step - 1]
        return total

    for n, dy in enumerate(NEAR_LAST):
        rotate_row(0, dy)
        if n == 0:
            pl.semaphore_wait(barrier, 14)
        send_row(0, dy)
    for dy in NEAR_LAST:
        rotate_row(1, dy)
    reduce_first(0, 2)
    reduce_first(0, 1)
    send_row(1, 2)
    reduce_first(0, 3)
    reduce_first(0, 0)
    for dy in NEAR_LAST[1:]:
        send_row(1, dy)
    for h in range(2):
        pair[h] = reduce_second(0, h)
        send_c(h).start()
    for step in NEAR_LAST:
        reduce_first(1, step)
    for h in range(2):
        first = reduce_second(1, h)
        send_c(h).wait_recv()
        decoded = encode(first + got_c[h])
        recoded[:, h] = decoded.T.astype(jnp.bfloat16).reshape(8, 16, QGROUP)
    for step in range(1, 8):
        send_n(step).start()
    own_copy.wait()
    second = [recoded[node, h].astype(jnp.float32) for h in range(2)]
    for step in range(1, 8):
        send_n(step).wait_recv()
        for h in range(2):
            second[h] += got_n[step - 1, h].astype(jnp.float32)

    lane = lax.broadcasted_iota(jnp.int32, (16, 32), 1)
    block = lax.broadcasted_iota(jnp.int32, (16, 32), 0)
    widest = jnp.zeros((1, 32), jnp.float32)
    for h in range(2):
        most = jnp.max(jnp.abs(second[h]), axis=1, keepdims=True) * (1.0 / 16.0)
        widest += jnp.sum(jnp.where(lane == 2 * block + h, most, 0.0), axis=0, keepdims=True)
    max_ref[...] = widest

    whole = jnp.concatenate(second, axis=1)
    high = whole.astype(jnp.bfloat16)
    rest = whole - high.astype(jnp.float32)
    middle = rest.astype(jnp.bfloat16)
    low = (rest - middle.astype(jnp.float32)).astype(jnp.bfloat16)
    pieces = jnp.concatenate([high, middle, low], axis=0)
    back = jnp.dot(pieces, matrix[...], preferred_element_type=jnp.float32)
    back = ((back[32:48] + back[16:32]) + back[0:16]) * (1.0 / ROT)
    for h in range(2):
        s = own_signs[pl.ds(h, 16, 2), :]
        half = back[:, h * QGROUP : (h + 1) * QGROUP]
        out_ref[pl.ds(h, 16, 2), :] = jnp.where(s == 0, half, -half)

    for own in range(2):
        for h in range(2):
            for step in range(1, 4):
                for c in range(4):
                    send_a(own, h, c, step).wait_send()
                send_b(own, h, step).wait_send()
    for h in range(2):
        send_c(h).wait_send()
    for step in range(1, 8):
        send_n(step).wait_send()


def shards(partials, signs):
    dma = pltpu.SemaphoreType.DMA
    out, widest = pl.pallas_call(
        kernel,
        out_shape=(
            jax.ShapeDtypeStruct((32, QGROUP), jnp.float32),
            jax.ShapeDtypeStruct((1, 32), jnp.float32),
        ),
        in_specs=[pl.BlockSpec(memory_space=pl.ANY)] * 2,
        out_specs=(
            pl.BlockSpec(memory_space=pltpu.VMEM),
            pl.BlockSpec(memory_space=pltpu.VMEM),
        ),
        scratch_shapes=[
            pltpu.VMEM((32, 8, 1, 4096), jnp.bfloat16),
            pltpu.VMEM((32, 8, 32, QGROUP), jnp.int32),
            pltpu.VMEM((32, QGROUP), jnp.int32),
            pltpu.VMEM((ROT, ROT), jnp.bfloat16),
            pltpu.VMEM((4, ROT, QGROUP), jnp.float32),
            pltpu.VMEM((2, 2, 4, 4, QGROUP, QGROUP), jnp.bfloat16),
            pltpu.VMEM((2, 2, 4, 3, QGROUP, QGROUP), jnp.bfloat16),
            pltpu.VMEM((2, 2, 4, QGROUP, QGROUP), jnp.float32),
            pltpu.VMEM((2, 2, 3, QGROUP, QGROUP), jnp.float32),
            pltpu.VMEM((2, QGROUP, QGROUP), jnp.float32),
            pltpu.VMEM((2, QGROUP, QGROUP), jnp.float32),
            pltpu.VMEM((8, 2, 16, QGROUP), jnp.bfloat16),
            pltpu.VMEM((7, 2, 16, QGROUP), jnp.bfloat16),
            dma((2, 33)),
            dma((2, 2, 4, 3)),
            dma((2, 2, 4, 3)),
            dma((2, 2, 3)),
            dma((2, 2, 3)),
            dma((2,)),
            dma((2,)),
            dma((7,)),
            dma((7,)),
        ],
        compiler_params=pltpu.CompilerParams(collective_id=0, has_side_effects=True),
    )(partials.reshape(8, 32, 1, 4096), signs.reshape(8, 32, 32, QGROUP))
    return out.reshape(-1), widest.reshape(-1)


def solution(mesh):
    in_specs = (P("node", "local", None), P())
    out_specs = (P(("node", "local")), P(("node", "local")))
    return jax.shard_map(shards, mesh=mesh, in_specs=in_specs, out_specs=out_specs, check_vma=False)
```

```python
import functools

import jax
import jax.numpy as jnp
from jax import lax
from jax.experimental import pallas as pl
from jax.experimental.pallas import tpu as pltpu
from jax.sharding import PartitionSpec as P

ROT = 256
QGROUP = 128
MESH = pl.DeviceIdType.MESH
NEAR_LAST = (2, 1, 3, 0)
FAR_FIRST = (6, 7, 4, 5, 2, 3, 1)


def power_below(values):
    lifted = values * 2.0**23
    nearest = (values + lifted) - lifted
    return jnp.where(nearest > values, 0.5 * nearest, nearest)


def encode(values):
    largest = jnp.max(jnp.abs(values), axis=0, keepdims=True)
    power = power_below(jnp.clip(largest, 2.0**-30, 1.5 * 2.0**30))
    inverse = 1.0 / power
    lifted = inverse * 2.0**23
    inverse = (inverse + lifted) - lifted
    units = jnp.trunc(values * (inverse * 2.0**17))
    anchor = jnp.maximum(jnp.abs(units) * 2.0**20, 1.5 * 2.0**24)
    code = (units * (1.0 + 2.0**-20) + anchor) - anchor
    return code * (power * 2.0**-17)


def kernel(
    x_hbm,
    signs_hbm,
    out_ref,
    max_ref,
    x_in,
    signs_in,
    own_signs,
    matrix,
    rows,
    coded,
    got_a,
    part,
    got_b,
    pair,
    got_c,
    recoded,
    got_n,
    in_sem,
    a_send,
    a_recv,
    b_send,
    b_recv,
    c_send,
    c_recv,
    n_send,
    n_recv,
):
    node, local = lax.axis_index("node"), lax.axis_index("local")
    me_y, me_x, me_z = local // 8, lax.rem(local // 2, 4), lax.rem(local, 2)

    def ahead(place, step):
        return lax.rem(place + step, 4)

    def device(y, x, z):
        return (node, y * 8 + x * 2 + z)

    def place_z(own):
        return me_z if own else 1 - me_z

    first_of = (me_x, me_y)
    second_of = (me_y, me_x)

    def along_first(h, step):
        if h == 0:
            return device(me_y, ahead(me_x, step), me_z)
        return device(ahead(me_y, step), me_x, me_z)

    def along_second(h, step):
        return along_first(1 - h, step)

    barrier = pltpu.get_barrier_semaphore()
    for h in range(2):
        for step in range(1, 4):
            pl.semaphore_signal(barrier, inc=1, device_id=along_first(h, step), device_id_type=MESH)
    pl.semaphore_signal(barrier, inc=1, device_id=device(me_y, me_x, 1 - me_z), device_id_type=MESH)
    for step in range(1, 8):
        pl.semaphore_signal(
            barrier, inc=1, device_id=(lax.rem(node + step, 8), local), device_id_type=MESH
        )

    def tile_of(own, dy, dx):
        return ahead(me_y, dy) * 8 + ahead(me_x, dx) * 2 + place_z(own)

    def load(own, dy, dx):
        t = tile_of(own, dy, dx)
        return (
            pltpu.make_async_copy(x_hbm.at[:, t], x_in.at[t], in_sem.at[0, t]),
            pltpu.make_async_copy(signs_hbm.at[:, t], signs_in.at[t], in_sem.at[1, t]),
        )

    def start_loads(own, dy):
        for dx in NEAR_LAST:
            for copy in load(own, dy, dx):
                copy.start()

    start_loads(0, NEAR_LAST[0])
    own_copy = pltpu.make_async_copy(signs_hbm.at[node, local], own_signs, in_sem.at[0, 32])
    own_copy.start()

    i = lax.broadcasted_iota(jnp.int32, (ROT, ROT), 0)
    j = lax.broadcasted_iota(jnp.int32, (ROT, ROT), 1)
    odd = lax.population_count(i & j) & 1
    matrix[...] = (1 - 2 * odd).astype(jnp.float32).astype(jnp.bfloat16)

    def send_a(own, h, c, step):
        return pltpu.make_async_remote_copy(
            src_ref=coded.at[h, own, c, ahead(first_of[h], step)],
            dst_ref=got_a.at[h, own, c, step - 1],
            send_sem=a_send.at[h, own, c, step - 1],
            recv_sem=a_recv.at[h, own, c, step - 1],
            device_id=along_first(h, step),
            device_id_type=MESH,
        )

    def send_b(own, h, step):
        return pltpu.make_async_remote_copy(
            src_ref=part.at[h, own, ahead(second_of[h], step)],
            dst_ref=got_b.at[h, own, step - 1],
            send_sem=b_send.at[h, own, step - 1],
            recv_sem=b_recv.at[h, own, step - 1],
            device_id=along_second(h, step),
            device_id_type=MESH,
        )

    def send_c(h):
        return pltpu.make_async_remote_copy(
            src_ref=pair.at[h],
            dst_ref=got_c.at[h],
            send_sem=c_send.at[h],
            recv_sem=c_recv.at[h],
            device_id=device(me_y, me_x, 1 - me_z),
            device_id_type=MESH,
        )

    def send_n(h, k):
        z, core = node // 2, lax.rem(node, 2)
        if k & 4:
            z = lax.rem(z + 2, 4)
        if k & 2:
            z = z + 1 - 2 * lax.rem(z, 2)
        if k & 1:
            core = 1 - core
        to = 2 * z + core
        return pltpu.make_async_remote_copy(
            src_ref=recoded.at[to, h],
            dst_ref=got_n.at[k - 1, h],
            send_sem=n_send.at[h, k - 1],
            recv_sem=n_recv.at[h, k - 1],
            device_id=(to, local),
            device_id_type=MESH,
        )

    def rotate(own, dy, steps):
        for dx in steps:
            for copy in load(own, dy, dx):
                copy.wait()
        for k, dx in enumerate(steps):
            t = tile_of(own, dy, dx)
            for g in range(8):
                for q in range(4):
                    v = x_in[t, g, :, pl.ds(q * 1024, 1024)].astype(jnp.float32).reshape(8, 128)
                    s = signs_in[t, g, pl.ds(q * 8, 8), :]
                    rows[k, pl.ds(g * 32 + q * 8, 8), :] = jnp.where(s == 0, v, -v)
        for k, dx in enumerate(steps):
            blocks = jnp.concatenate(
                [
                    rows[k, pl.ds(0, 128, 2), :].astype(jnp.bfloat16),
                    rows[k, pl.ds(1, 128, 2), :].astype(jnp.bfloat16),
                ],
                axis=1,
            )
            rotated = lax.dot_general(
                matrix[...],
                blocks,
                (((1,), (1,)), ((), ())),
                preferred_element_type=jnp.float32,
            )
            y, x = ahead(me_y, dy), ahead(me_x, dx)
            coded[0, own, y, x] = encode(rotated[:QGROUP]).astype(jnp.bfloat16)
            coded[1, own, x, y] = encode(rotated[QGROUP:]).astype(jnp.bfloat16)

    def send_tiles(own, dy, steps=NEAR_LAST):
        for dx in steps:
            if dx:
                send_a(own, 0, ahead(me_y, dy), dx).start()
            if dy:
                send_a(own, 1, ahead(me_x, dx), dy).start()

    def add_first(own, h, c):
        for step in range(1, 4):
            send_a(own, h, c, step).wait_recv()
        total = coded[h, own, c, first_of[h]].astype(jnp.float32)
        for step in range(1, 4):
            total += got_a[h, own, c, step - 1].astype(jnp.float32)
        return total

    def reduce_first(own, step):
        for h in range(2):
            c = ahead(second_of[h], step)
            part[h, own, c] = add_first(own, h, c)
            if step:
                send_b(own, h, step).start()

    def reduce_second(own, h):
        for step in range(1, 4):
            send_b(own, h, step).wait_recv()
        total = part[h, own, second_of[h]]
        for step in range(1, 4):
            total += got_b[h, own, step - 1]
        return total

    first_row, *other_rows = NEAR_LAST
    rotate(0, first_row, NEAR_LAST[:2])
    for own in range(2):
        for dy in other_rows if own == 0 else NEAR_LAST:
            start_loads(own, dy)
    pl.semaphore_wait(barrier, 14)
    send_tiles(0, first_row, NEAR_LAST[:2])
    rotate(0, first_row, NEAR_LAST[2:])
    send_tiles(0, first_row, NEAR_LAST[2:])
    for dy in other_rows:
        rotate(0, dy, NEAR_LAST)
        send_tiles(0, dy)
    for dy in NEAR_LAST:
        rotate(1, dy, NEAR_LAST)
    reduce_first(0, 2)
    reduce_first(0, 1)
    send_tiles(1, 2)
    reduce_first(0, 3)
    reduce_first(0, 0)
    for dy in NEAR_LAST[1:]:
        send_tiles(1, dy)
    for h in range(2):
        pair[h] = reduce_second(0, h)
        send_c(h).start()
    for step in NEAR_LAST:
        reduce_first(1, step)
    for h in range(2):
        first = reduce_second(1, h)
        send_c(h).wait_recv()
        decoded = encode(first + got_c[h])
        recoded[:, h] = decoded.T.astype(jnp.bfloat16).reshape(8, 16, QGROUP)
        for k in FAR_FIRST:
            send_n(h, k).start()
    own_copy.wait()
    for own in range(2):
        for h in range(2):
            for step in range(1, 4):
                for c in range(4):
                    send_a(own, h, c, step).wait_send()
                send_b(own, h, step).wait_send()
    for h in range(2):
        send_c(h).wait_send()
    second = [recoded[node, h].astype(jnp.float32) for h in range(2)]
    for h in range(2):
        for k in reversed(FAR_FIRST):
            send_n(h, k).wait_recv()
            second[h] += got_n[k - 1, h].astype(jnp.float32)

    lane = lax.broadcasted_iota(jnp.int32, (16, 32), 1)
    block = lax.broadcasted_iota(jnp.int32, (16, 32), 0)
    widest = jnp.zeros((1, 32), jnp.float32)
    for h in range(2):
        most = jnp.max(jnp.abs(second[h]), axis=1, keepdims=True)
        widest += jnp.sum(jnp.where(lane == 2 * block + h, most, 0.0), axis=0, keepdims=True)
    max_ref[...] = widest

    whole = jnp.concatenate(second, axis=1)
    high = whole.astype(jnp.bfloat16)
    rest = whole - high.astype(jnp.float32)
    middle = rest.astype(jnp.bfloat16)
    low = (rest - middle.astype(jnp.float32)).astype(jnp.bfloat16)
    pieces = jnp.concatenate([high, middle, low], axis=0)
    back = jnp.dot(pieces, matrix[...], preferred_element_type=jnp.float32)
    back = (back[32:48] + back[16:32]) + back[0:16]
    for h in range(2):
        s = own_signs[pl.ds(h, 16, 2), :]
        half = back[:, h * QGROUP : (h + 1) * QGROUP]
        out_ref[pl.ds(h, 16, 2), :] = jnp.where(s == 0, half, -half)

    for h in range(2):
        for k in FAR_FIRST:
            send_n(h, k).wait_send()


def finish(turned_ref, most_ref, out_ref, max_ref):
    out_ref[...] = turned_ref[...] * (1.0 / ROT)
    max_ref[...] = most_ref[...] * (1.0 / 16.0)


def shards(partials, signs):
    dma = pltpu.SemaphoreType.DMA
    shapes = (
        jax.ShapeDtypeStruct((32, QGROUP), jnp.float32),
        jax.ShapeDtypeStruct((1, 32), jnp.float32),
    )
    turned, most = pl.pallas_call(
        kernel,
        out_shape=shapes,
        in_specs=[pl.BlockSpec(memory_space=pl.ANY)] * 2,
        out_specs=(
            pl.BlockSpec(memory_space=pltpu.VMEM),
            pl.BlockSpec(memory_space=pltpu.VMEM),
        ),
        scratch_shapes=[
            pltpu.VMEM((32, 8, 1, 4096), jnp.bfloat16),
            pltpu.VMEM((32, 8, 32, QGROUP), jnp.int32),
            pltpu.VMEM((32, QGROUP), jnp.int32),
            pltpu.VMEM((ROT, ROT), jnp.bfloat16),
            pltpu.VMEM((4, ROT, QGROUP), jnp.float32),
            pltpu.VMEM((2, 2, 4, 4, QGROUP, QGROUP), jnp.bfloat16),
            pltpu.VMEM((2, 2, 4, 3, QGROUP, QGROUP), jnp.bfloat16),
            pltpu.VMEM((2, 2, 4, QGROUP, QGROUP), jnp.float32),
            pltpu.VMEM((2, 2, 3, QGROUP, QGROUP), jnp.float32),
            pltpu.VMEM((2, QGROUP, QGROUP), jnp.float32),
            pltpu.VMEM((2, QGROUP, QGROUP), jnp.float32),
            pltpu.VMEM((8, 2, 16, QGROUP), jnp.bfloat16),
            pltpu.VMEM((7, 2, 16, QGROUP), jnp.bfloat16),
            dma((2, 33)),
            dma((2, 2, 4, 3)),
            dma((2, 2, 4, 3)),
            dma((2, 2, 3)),
            dma((2, 2, 3)),
            dma((2,)),
            dma((2,)),
            dma((2, 7)),
            dma((2, 7)),
        ],
        compiler_params=pltpu.CompilerParams(collective_id=0, has_side_effects=True),
    )(partials.reshape(8, 32, 1, 4096), signs.reshape(8, 32, 32, QGROUP))
    out, widest = pl.pallas_call(finish, out_shape=shapes)(turned, most)
    return out.reshape(-1), widest.reshape(-1)


def solution(mesh):
    in_specs = (P("node", "local", None), P())
    out_specs = (P(("node", "local")), P(("node", "local")))
    return jax.shard_map(shards, mesh=mesh, in_specs=in_specs, out_specs=out_specs, check_vma=False)
```

```python
import functools

import jax
import jax.numpy as jnp
from jax import lax
from jax.experimental import pallas as pl
from jax.experimental.pallas import tpu as pltpu
from jax.sharding import PartitionSpec as P

ROT = 256
QGROUP = 128
MESH = pl.DeviceIdType.MESH
NEAR_LAST = (2, 1, 3, 0)
LOADS = ((0, 2), (2, 4), (4, 8), (8, 12), (12, 16), (16, 32))
FAR_FIRST = (6, 7, 4, 5, 2, 3, 1)


def power_below(values):
    lifted = values * 2.0**23
    nearest = (values + lifted) - lifted
    return jnp.where(nearest > values, 0.5 * nearest, nearest)


def encode(values):
    largest = jnp.max(jnp.abs(values), axis=0, keepdims=True)
    power = power_below(jnp.clip(largest, 2.0**-30, 1.5 * 2.0**30))
    inverse = 1.0 / power
    lifted = inverse * 2.0**23
    inverse = (inverse + lifted) - lifted
    units = jnp.trunc(values * (inverse * 2.0**17))
    anchor = jnp.maximum(jnp.abs(units) * 2.0**20, 1.5 * 2.0**24)
    code = (units * (1.0 + 2.0**-20) + anchor) - anchor
    return code * (power * 2.0**-17)


def kernel(
    x_hbm,
    signs_hbm,
    out_ref,
    max_ref,
    x_in,
    signs_in,
    own_signs,
    matrix,
    rows,
    coded,
    got_a,
    part,
    got_b,
    pair,
    got_c,
    recoded,
    got_n,
    in_sem,
    a_send,
    a_recv,
    b_send,
    b_recv,
    c_send,
    c_recv,
    n_send,
    n_recv,
):
    node, local = lax.axis_index("node"), lax.axis_index("local")
    me_y, me_x, me_z = local // 8, lax.rem(local // 2, 4), lax.rem(local, 2)

    def ahead(place, step):
        return lax.rem(place + step, 4)

    def device(y, x, z):
        return (node, y * 8 + x * 2 + z)

    def place_z(own):
        return me_z if own else 1 - me_z

    first_of = (me_x, me_y)
    second_of = (me_y, me_x)

    def along_first(h, step):
        if h == 0:
            return device(me_y, ahead(me_x, step), me_z)
        return device(ahead(me_y, step), me_x, me_z)

    def along_second(h, step):
        return along_first(1 - h, step)

    barrier = pltpu.get_barrier_semaphore()
    for h in range(2):
        for step in range(1, 4):
            pl.semaphore_signal(barrier, inc=1, device_id=along_first(h, step), device_id_type=MESH)
    pl.semaphore_signal(barrier, inc=1, device_id=device(me_y, me_x, 1 - me_z), device_id_type=MESH)
    for step in range(1, 8):
        pl.semaphore_signal(
            barrier, inc=1, device_id=(lax.rem(node + step, 8), local), device_id_type=MESH
        )

    def tile_of(own, dy, dx):
        return ahead(me_y, dy) * 8 + ahead(me_x, dx) * 2 + place_z(own)

    def slot_of(own, dy, dx):
        return 16 * own + 4 * NEAR_LAST.index(dy) + NEAR_LAST.index(dx)

    def start_loads(group):
        first, last = LOADS[group]
        for slot in range(first, last):
            own, dy, dx = slot // 16, NEAR_LAST[slot // 4 % 4], NEAR_LAST[slot % 4]
            t = tile_of(own, dy, dx)
            pltpu.make_async_copy(x_hbm.at[:, t], x_in.at[slot], in_sem.at[0, group]).start()
            pltpu.make_async_copy(
                signs_hbm.at[:, t], signs_in.at[slot], in_sem.at[1, group]
            ).start()

    def wait_loads(group):
        first, last = LOADS[group]
        for n, buffer in enumerate((x_in, signs_in)):
            whole = buffer.at[pl.ds(first, last - first)]
            pltpu.make_async_copy(whole, whole, in_sem.at[n, group]).wait()

    start_loads(0)
    own_copy = pltpu.make_async_copy(signs_hbm.at[node, local], own_signs, in_sem.at[0, len(LOADS)])
    own_copy.start()

    i = lax.broadcasted_iota(jnp.int32, (ROT, ROT), 0)
    j = lax.broadcasted_iota(jnp.int32, (ROT, ROT), 1)
    odd = lax.population_count(i & j) & 1
    matrix[...] = (1 - 2 * odd).astype(jnp.float32).astype(jnp.bfloat16)

    def send_a(own, h, c, step):
        return pltpu.make_async_remote_copy(
            src_ref=coded.at[h, own, c, ahead(first_of[h], step)],
            dst_ref=got_a.at[h, own, c, step - 1],
            send_sem=a_send,
            recv_sem=a_recv.at[h, own, c],
            device_id=along_first(h, step),
            device_id_type=MESH,
        )

    def send_b(own, h, step):
        return pltpu.make_async_remote_copy(
            src_ref=part.at[h, own, ahead(second_of[h], step)],
            dst_ref=got_b.at[h, own, step - 1],
            send_sem=b_send,
            recv_sem=b_recv.at[h, own],
            device_id=along_second(h, step),
            device_id_type=MESH,
        )

    def send_c(h):
        return pltpu.make_async_remote_copy(
            src_ref=pair.at[h],
            dst_ref=got_c.at[h],
            send_sem=c_send,
            recv_sem=c_recv.at[h],
            device_id=device(me_y, me_x, 1 - me_z),
            device_id_type=MESH,
        )

    def send_n(h, k):
        z, core = node // 2, lax.rem(node, 2)
        if k & 4:
            z = lax.rem(z + 2, 4)
        if k & 2:
            z = z + 1 - 2 * lax.rem(z, 2)
        if k & 1:
            core = 1 - core
        to = 2 * z + core
        return pltpu.make_async_remote_copy(
            src_ref=recoded.at[to, h],
            dst_ref=got_n.at[h, k - 1],
            send_sem=n_send,
            recv_sem=n_recv.at[h],
            device_id=(to, local),
            device_id_type=MESH,
        )

    def rotate(own, dy, steps):
        for k, dx in enumerate(steps):
            t = slot_of(own, dy, dx)
            for g in range(8):
                for q in range(4):
                    v = x_in[t, g, :, pl.ds(q * 1024, 1024)].astype(jnp.float32).reshape(8, 128)
                    s = signs_in[t, g, pl.ds(q * 8, 8), :]
                    rows[k, pl.ds(g * 32 + q * 8, 8), :] = jnp.where(s == 0, v, -v)
        for k, dx in enumerate(steps):
            blocks = jnp.concatenate(
                [
                    rows[k, pl.ds(0, 128, 2), :].astype(jnp.bfloat16),
                    rows[k, pl.ds(1, 128, 2), :].astype(jnp.bfloat16),
                ],
                axis=1,
            )
            rotated = lax.dot_general(
                matrix[...],
                blocks,
                (((1,), (1,)), ((), ())),
                preferred_element_type=jnp.float32,
            )
            y, x = ahead(me_y, dy), ahead(me_x, dx)
            coded[0, own, y, x] = encode(rotated[:QGROUP]).astype(jnp.bfloat16)
            coded[1, own, x, y] = encode(rotated[QGROUP:]).astype(jnp.bfloat16)

    def send_tiles(own, dy, steps=NEAR_LAST):
        for dx in steps:
            if dx:
                send_a(own, 0, ahead(me_y, dy), dx).start()
            if dy:
                send_a(own, 1, ahead(me_x, dx), dy).start()

    def wait_for(buffer, sem):
        pltpu.make_async_copy(buffer, buffer, sem).wait()

    def add_first(own, h, c):
        wait_for(got_a.at[h, own, c], a_recv.at[h, own, c])
        total = coded[h, own, c, first_of[h]].astype(jnp.float32)
        for step in range(1, 4):
            total += got_a[h, own, c, step - 1].astype(jnp.float32)
        return total

    def reduce_first(own, step):
        for h in range(2):
            c = ahead(second_of[h], step)
            part[h, own, c] = add_first(own, h, c)
            if step:
                send_b(own, h, step).start()

    def reduce_second(own, h):
        wait_for(got_b.at[h, own], b_recv.at[h, own])
        total = part[h, own, second_of[h]]
        for step in range(1, 4):
            total += got_b[h, own, step - 1]
        return total

    first_row, *other_rows = NEAR_LAST
    wait_loads(0)
    rotate(0, first_row, NEAR_LAST[:2])
    for group in range(1, len(LOADS)):
        start_loads(group)
    pl.semaphore_wait(barrier, 14)
    send_tiles(0, first_row, NEAR_LAST[:2])
    wait_loads(1)
    rotate(0, first_row, NEAR_LAST[2:])
    send_tiles(0, first_row, NEAR_LAST[2:])
    for n, dy in enumerate(other_rows):
        wait_loads(2 + n)
        rotate(0, dy, NEAR_LAST)
        send_tiles(0, dy)
    wait_loads(5)
    for dy in NEAR_LAST:
        rotate(1, dy, NEAR_LAST)
    reduce_first(0, 2)
    reduce_first(0, 1)
    send_tiles(1, 2)
    reduce_first(0, 3)
    reduce_first(0, 0)
    for dy in NEAR_LAST[1:]:
        send_tiles(1, dy)
    for h in range(2):
        pair[h] = reduce_second(0, h)
        send_c(h).start()
    for step in NEAR_LAST:
        reduce_first(1, step)
    for h in range(2):
        first = reduce_second(1, h)
        wait_for(got_c.at[h], c_recv.at[h])
        decoded = encode(first + got_c[h])
        recoded[:, h] = decoded.T.astype(jnp.bfloat16).reshape(8, 16, QGROUP)
        for k in FAR_FIRST:
            send_n(h, k).start()
    own_copy.wait()
    wait_for(got_a, a_send)
    wait_for(got_b, b_send)
    wait_for(got_c, c_send)
    second = [recoded[node, h].astype(jnp.float32) for h in range(2)]
    for h in range(2):
        wait_for(got_n.at[h], n_recv.at[h])
        for k in reversed(FAR_FIRST):
            second[h] += got_n[h, k - 1].astype(jnp.float32)

    lane = lax.broadcasted_iota(jnp.int32, (16, 32), 1)
    block = lax.broadcasted_iota(jnp.int32, (16, 32), 0)
    widest = jnp.zeros((1, 32), jnp.float32)
    for h in range(2):
        most = jnp.max(jnp.abs(second[h]), axis=1, keepdims=True) * (1.0 / 16.0)
        widest += jnp.sum(jnp.where(lane == 2 * block + h, most, 0.0), axis=0, keepdims=True)
    max_ref[...] = widest

    whole = jnp.concatenate(second, axis=1)
    high = whole.astype(jnp.bfloat16)
    rest = whole - high.astype(jnp.float32)
    middle = rest.astype(jnp.bfloat16)
    low = (rest - middle.astype(jnp.float32)).astype(jnp.bfloat16)
    pieces = jnp.concatenate([high, middle, low], axis=0)
    back = jnp.dot(pieces, matrix[...], preferred_element_type=jnp.float32)
    back = ((back[32:48] + back[16:32]) + back[0:16]) * (1.0 / ROT)
    for h in range(2):
        s = own_signs[pl.ds(h, 16, 2), :]
        half = back[:, h * QGROUP : (h + 1) * QGROUP]
        out_ref[pl.ds(h, 16, 2), :] = jnp.where(s == 0, half, -half)

    wait_for(got_n, n_send)


def finish(turned_ref, most_ref, out_ref, max_ref, sem):
    copies = (
        pltpu.make_async_copy(turned_ref, out_ref, sem.at[0]),
        pltpu.make_async_copy(most_ref, max_ref, sem.at[1]),
    )
    for copy in copies:
        copy.start()
    for copy in copies:
        copy.wait()


def shards(partials, signs):
    dma = pltpu.SemaphoreType.DMA
    turned, most = pl.pallas_call(
        kernel,
        out_shape=(pltpu.VMEM((32, QGROUP), jnp.float32), pltpu.VMEM((1, 32), jnp.float32)),
        in_specs=[pl.BlockSpec(memory_space=pl.ANY)] * 2,
        out_specs=(
            pl.BlockSpec(memory_space=pltpu.VMEM),
            pl.BlockSpec(memory_space=pltpu.VMEM),
        ),
        scratch_shapes=[
            pltpu.VMEM((32, 8, 1, 4096), jnp.bfloat16),
            pltpu.VMEM((32, 8, 32, QGROUP), jnp.int32),
            pltpu.VMEM((32, QGROUP), jnp.int32),
            pltpu.VMEM((ROT, ROT), jnp.bfloat16),
            pltpu.VMEM((4, ROT, QGROUP), jnp.float32),
            pltpu.VMEM((2, 2, 4, 4, QGROUP, QGROUP), jnp.bfloat16),
            pltpu.VMEM((2, 2, 4, 3, QGROUP, QGROUP), jnp.bfloat16),
            pltpu.VMEM((2, 2, 4, QGROUP, QGROUP), jnp.float32),
            pltpu.VMEM((2, 2, 3, QGROUP, QGROUP), jnp.float32),
            pltpu.VMEM((2, QGROUP, QGROUP), jnp.float32),
            pltpu.VMEM((2, QGROUP, QGROUP), jnp.float32),
            pltpu.VMEM((8, 2, 16, QGROUP), jnp.bfloat16),
            pltpu.VMEM((2, 7, 16, QGROUP), jnp.bfloat16),
            dma((2, len(LOADS) + 1)),
            dma,
            dma((2, 2, 4)),
            dma,
            dma((2, 2)),
            dma,
            dma((2,)),
            dma,
            dma((2,)),
        ],
        compiler_params=pltpu.CompilerParams(collective_id=0, has_side_effects=True),
    )(partials.reshape(8, 32, 1, 4096), signs.reshape(8, 32, 32, QGROUP))
    out, widest = pl.pallas_call(
        finish,
        out_shape=(
            jax.ShapeDtypeStruct((32, QGROUP), jnp.float32),
            jax.ShapeDtypeStruct((1, 32), jnp.float32),
        ),
        in_specs=[pl.BlockSpec(memory_space=pltpu.VMEM)] * 2,
        out_specs=[pl.BlockSpec(memory_space=pl.ANY)] * 2,
        scratch_shapes=[dma((2,))],
    )(
        pltpu.with_memory_space_constraint(turned, pltpu.VMEM),
        pltpu.with_memory_space_constraint(most, pltpu.VMEM),
    )
    return out.reshape(-1), widest.reshape(-1)


def solution(mesh):
    in_specs = (P("node", "local", None), P())
    out_specs = (P(("node", "local")), P(("node", "local")))
    return jax.shard_map(shards, mesh=mesh, in_specs=in_specs, out_specs=out_specs, check_vma=False)
```

```python
import functools

import jax
import jax.numpy as jnp
from jax import lax
from jax.experimental import pallas as pl
from jax.experimental.pallas import tpu as pltpu
from jax.sharding import PartitionSpec as P

ROT = 256
QGROUP = 128
MESH = pl.DeviceIdType.MESH
NEAR_LAST = (2, 1, 3, 0)
LOADS = ((0, 2), (2, 4), (4, 8), (8, 12), (12, 16), (16, 32))
PARTS = ((0, 0, 64), (0, 64, 64), (1, 0, 128))
FAR_FIRST = (6, 7, 4, 5, 2, 3, 1)


def power_below(values):
    lifted = values * 2.0**23
    nearest = (values + lifted) - lifted
    return jnp.where(nearest > values, 0.5 * nearest, nearest)


def encode(values):
    largest = jnp.max(jnp.abs(values), axis=0, keepdims=True)
    power = power_below(jnp.clip(largest, 2.0**-30, 1.5 * 2.0**30))
    inverse = 1.0 / power
    lifted = inverse * 2.0**23
    inverse = (inverse + lifted) - lifted
    units = jnp.trunc(values * (inverse * 2.0**17))
    anchor = jnp.maximum(jnp.abs(units) * 2.0**20, 1.5 * 2.0**24)
    code = (units * (1.0 + 2.0**-20) + anchor) - anchor
    return code * (power * 2.0**-17)


def kernel(
    x_hbm,
    signs_hbm,
    out_ref,
    max_ref,
    x_in,
    signs_in,
    own_signs,
    matrix,
    rows,
    coded,
    got_a,
    part,
    got_b,
    pair,
    got_c,
    recoded,
    got_n,
    in_sem,
    a_send,
    a_recv,
    b_send,
    b_recv,
    c_send,
    c_recv,
    n_send,
    n_recv,
):
    node, local = lax.axis_index("node"), lax.axis_index("local")
    me_y, me_x, me_z = local // 8, lax.rem(local // 2, 4), lax.rem(local, 2)

    def ahead(place, step):
        return lax.rem(place + step, 4)

    def device(y, x, z):
        return (node, y * 8 + x * 2 + z)

    def place_z(own):
        return me_z if own else 1 - me_z

    first_of = (me_x, me_y)
    second_of = (me_y, me_x)

    def along_first(h, step):
        if h == 0:
            return device(me_y, ahead(me_x, step), me_z)
        return device(ahead(me_y, step), me_x, me_z)

    def along_second(h, step):
        return along_first(1 - h, step)

    barrier = pltpu.get_barrier_semaphore()
    for h in range(2):
        for step in range(1, 4):
            pl.semaphore_signal(barrier, inc=1, device_id=along_first(h, step), device_id_type=MESH)
    pl.semaphore_signal(barrier, inc=1, device_id=device(me_y, me_x, 1 - me_z), device_id_type=MESH)
    for step in range(1, 8):
        pl.semaphore_signal(
            barrier, inc=1, device_id=(lax.rem(node + step, 8), local), device_id_type=MESH
        )

    def tile_of(own, dy, dx):
        return ahead(me_y, dy) * 8 + ahead(me_x, dx) * 2 + place_z(own)

    def slot_of(own, dy, dx):
        return 16 * own + 4 * NEAR_LAST.index(dy) + NEAR_LAST.index(dx)

    def start_loads(group):
        first, last = LOADS[group]
        for slot in range(first, last):
            own, dy, dx = slot // 16, NEAR_LAST[slot // 4 % 4], NEAR_LAST[slot % 4]
            t = tile_of(own, dy, dx)
            pltpu.make_async_copy(x_hbm.at[:, t], x_in.at[slot], in_sem.at[0, group]).start()
            pltpu.make_async_copy(
                signs_hbm.at[:, t], signs_in.at[slot], in_sem.at[1, group]
            ).start()

    def wait_loads(group):
        first, last = LOADS[group]
        for n, buffer in enumerate((x_in, signs_in)):
            whole = buffer.at[pl.ds(first, last - first)]
            pltpu.make_async_copy(whole, whole, in_sem.at[n, group]).wait()

    start_loads(0)
    own_copy = pltpu.make_async_copy(signs_hbm.at[node, local], own_signs, in_sem.at[0, len(LOADS)])
    own_copy.start()

    i = lax.broadcasted_iota(jnp.int32, (ROT, ROT), 0)
    j = lax.broadcasted_iota(jnp.int32, (ROT, ROT), 1)
    odd = lax.population_count(i & j) & 1
    matrix[...] = (1 - 2 * odd).astype(jnp.float32).astype(jnp.bfloat16)

    def rows_of(p):
        return pl.ds(PARTS[p][1], PARTS[p][2])

    def send_a(p, h, c, step):
        own = PARTS[p][0]
        return pltpu.make_async_remote_copy(
            src_ref=coded.at[h, own, c, ahead(first_of[h], step), rows_of(p)],
            dst_ref=got_a.at[h, own, c, step - 1, rows_of(p)],
            send_sem=a_send,
            recv_sem=a_recv.at[h, p, c],
            device_id=along_first(h, step),
            device_id_type=MESH,
        )

    def send_b(p, h, step):
        own = PARTS[p][0]
        return pltpu.make_async_remote_copy(
            src_ref=part.at[h, own, ahead(second_of[h], step), rows_of(p)],
            dst_ref=got_b.at[h, own, step - 1, rows_of(p)],
            send_sem=b_send,
            recv_sem=b_recv.at[h, p],
            device_id=along_second(h, step),
            device_id_type=MESH,
        )

    def send_c(p, h):
        return pltpu.make_async_remote_copy(
            src_ref=pair.at[h, rows_of(p)],
            dst_ref=got_c.at[h, rows_of(p)],
            send_sem=c_send,
            recv_sem=c_recv.at[h, p],
            device_id=device(me_y, me_x, 1 - me_z),
            device_id_type=MESH,
        )

    def send_n(h, k):
        z, core = node // 2, lax.rem(node, 2)
        if k & 4:
            z = lax.rem(z + 2, 4)
        if k & 2:
            z = z + 1 - 2 * lax.rem(z, 2)
        if k & 1:
            core = 1 - core
        to = 2 * z + core
        return pltpu.make_async_remote_copy(
            src_ref=recoded.at[to, h],
            dst_ref=got_n.at[h, k - 1],
            send_sem=n_send,
            recv_sem=n_recv.at[h],
            device_id=(to, local),
            device_id_type=MESH,
        )

    def rotate(own, dy, steps):
        for k, dx in enumerate(steps):
            t = slot_of(own, dy, dx)
            for g in range(8):
                for q in range(4):
                    v = x_in[t, g, :, pl.ds(q * 1024, 1024)].astype(jnp.float32).reshape(8, 128)
                    s = signs_in[t, g, pl.ds(q * 8, 8), :]
                    rows[k, pl.ds(g * 32 + q * 8, 8), :] = jnp.where(s == 0, v, -v)
        for k, dx in enumerate(steps):
            blocks = jnp.concatenate(
                [
                    rows[k, pl.ds(0, 128, 2), :].astype(jnp.bfloat16),
                    rows[k, pl.ds(1, 128, 2), :].astype(jnp.bfloat16),
                ],
                axis=1,
            )
            rotated = lax.dot_general(
                matrix[...],
                blocks,
                (((1,), (1,)), ((), ())),
                preferred_element_type=jnp.float32,
            )
            y, x = ahead(me_y, dy), ahead(me_x, dx)
            coded[0, own, y, x] = encode(rotated[:QGROUP]).astype(jnp.bfloat16)
            coded[1, own, x, y] = encode(rotated[QGROUP:]).astype(jnp.bfloat16)

    def send_tiles(dy, steps):
        for dx in steps:
            if dx:
                send_a(0, 0, ahead(me_y, dy), dx).start()
            if dy:
                send_a(0, 1, ahead(me_x, dx), dy).start()

    def send_chunk(p, step):
        for to in NEAR_LAST[:3]:
            for h in range(2):
                send_a(p, h, ahead(second_of[h], step), to).start()

    def wait_for(buffer, sem):
        pltpu.make_async_copy(buffer, buffer, sem).wait()

    def reduce_first(p, step):
        own, rows = PARTS[p][0], rows_of(p)
        for h in range(2):
            c = ahead(second_of[h], step)
            wait_for(got_a.at[h, own, c, pl.ds(0, 3), rows], a_recv.at[h, p, c])
            total = coded[h, own, c, first_of[h], rows].astype(jnp.float32)
            for k in range(3):
                total += got_a[h, own, c, k, rows].astype(jnp.float32)
            part[h, own, c, rows] = total
            if step:
                send_b(p, h, step).start()

    def reduce_second(p, h):
        own, rows = PARTS[p][0], rows_of(p)
        wait_for(got_b.at[h, own, pl.ds(0, 3), rows], b_recv.at[h, p])
        total = part[h, own, second_of[h], rows]
        for k in range(3):
            total += got_b[h, own, k, rows]
        return total

    def exchange_z(p):
        for h in range(2):
            pair[h, rows_of(p)] = reduce_second(p, h)
            send_c(p, h).start()

    first_row, *other_rows = NEAR_LAST
    wait_loads(0)
    rotate(0, first_row, NEAR_LAST[:2])
    for group in range(1, len(LOADS)):
        start_loads(group)
    pl.semaphore_wait(barrier, 14)
    send_tiles(first_row, NEAR_LAST[:2])
    wait_loads(1)
    rotate(0, first_row, NEAR_LAST[2:])
    send_tiles(first_row, NEAR_LAST[2:])
    for n, dy in enumerate(other_rows):
        wait_loads(2 + n)
        rotate(0, dy, NEAR_LAST)
        send_tiles(dy, NEAR_LAST)
    for step in NEAR_LAST:
        send_chunk(1, step)
    wait_loads(5)
    for dy in NEAR_LAST:
        rotate(1, dy, NEAR_LAST)
    for step in NEAR_LAST:
        reduce_first(0, step)
    send_chunk(2, 2)
    for step in NEAR_LAST:
        reduce_first(1, step)
    send_chunk(2, 1)
    exchange_z(0)
    send_chunk(2, 3)
    send_chunk(2, 0)
    exchange_z(1)
    for step in NEAR_LAST:
        reduce_first(2, step)
    for h in range(2):
        first = reduce_second(2, h)
        wait_for(got_c.at[h, rows_of(0)], c_recv.at[h, 0])
        wait_for(got_c.at[h, rows_of(1)], c_recv.at[h, 1])
        decoded = encode(first + got_c[h])
        recoded[:, h] = decoded.T.astype(jnp.bfloat16).reshape(8, 16, QGROUP)
        for k in FAR_FIRST:
            send_n(h, k).start()
    own_copy.wait()
    wait_for(got_a, a_send)
    wait_for(got_b, b_send)
    wait_for(got_c, c_send)
    second = [recoded[node, h].astype(jnp.float32) for h in range(2)]
    for h in range(2):
        wait_for(got_n.at[h], n_recv.at[h])
        for k in reversed(FAR_FIRST):
            second[h] += got_n[h, k - 1].astype(jnp.float32)

    lane = lax.broadcasted_iota(jnp.int32, (16, 32), 1)
    block = lax.broadcasted_iota(jnp.int32, (16, 32), 0)
    widest = jnp.zeros((1, 32), jnp.float32)
    for h in range(2):
        most = jnp.max(jnp.abs(second[h]), axis=1, keepdims=True) * (1.0 / 16.0)
        widest += jnp.sum(jnp.where(lane == 2 * block + h, most, 0.0), axis=0, keepdims=True)
    max_ref[...] = widest

    whole = jnp.concatenate(second, axis=1)
    high = whole.astype(jnp.bfloat16)
    rest = whole - high.astype(jnp.float32)
    middle = rest.astype(jnp.bfloat16)
    low = (rest - middle.astype(jnp.float32)).astype(jnp.bfloat16)
    pieces = jnp.concatenate([high, middle, low], axis=0)
    back = jnp.dot(pieces, matrix[...], preferred_element_type=jnp.float32)
    back = ((back[32:48] + back[16:32]) + back[0:16]) * (1.0 / ROT)
    for h in range(2):
        s = own_signs[pl.ds(h, 16, 2), :]
        half = back[:, h * QGROUP : (h + 1) * QGROUP]
        out_ref[pl.ds(h, 16, 2), :] = jnp.where(s == 0, half, -half)

    wait_for(got_n, n_send)


def finish(turned_ref, most_ref, out_ref, max_ref, sem):
    copies = (
        pltpu.make_async_copy(turned_ref, out_ref, sem.at[0]),
        pltpu.make_async_copy(most_ref, max_ref, sem.at[1]),
    )
    for copy in copies:
        copy.start()
    for copy in copies:
        copy.wait()


def shards(partials, signs):
    dma = pltpu.SemaphoreType.DMA
    turned, most = pl.pallas_call(
        kernel,
        out_shape=(pltpu.VMEM((32, QGROUP), jnp.float32), pltpu.VMEM((1, 32), jnp.float32)),
        in_specs=[pl.BlockSpec(memory_space=pl.ANY)] * 2,
        out_specs=(
            pl.BlockSpec(memory_space=pltpu.VMEM),
            pl.BlockSpec(memory_space=pltpu.VMEM),
        ),
        scratch_shapes=[
            pltpu.VMEM((32, 8, 1, 4096), jnp.bfloat16),
            pltpu.VMEM((32, 8, 32, QGROUP), jnp.int32),
            pltpu.VMEM((32, QGROUP), jnp.int32),
            pltpu.VMEM((ROT, ROT), jnp.bfloat16),
            pltpu.VMEM((4, ROT, QGROUP), jnp.float32),
            pltpu.VMEM((2, 2, 4, 4, QGROUP, QGROUP), jnp.bfloat16),
            pltpu.VMEM((2, 2, 4, 3, QGROUP, QGROUP), jnp.bfloat16),
            pltpu.VMEM((2, 2, 4, QGROUP, QGROUP), jnp.float32),
            pltpu.VMEM((2, 2, 3, QGROUP, QGROUP), jnp.float32),
            pltpu.VMEM((2, QGROUP, QGROUP), jnp.float32),
            pltpu.VMEM((2, QGROUP, QGROUP), jnp.float32),
            pltpu.VMEM((8, 2, 16, QGROUP), jnp.bfloat16),
            pltpu.VMEM((2, 7, 16, QGROUP), jnp.bfloat16),
            dma((2, len(LOADS) + 1)),
            dma,
            dma((2, 3, 4)),
            dma,
            dma((2, 3)),
            dma,
            dma((2, 2)),
            dma,
            dma((2,)),
        ],
        compiler_params=pltpu.CompilerParams(collective_id=0, has_side_effects=True),
    )(partials.reshape(8, 32, 1, 4096), signs.reshape(8, 32, 32, QGROUP))
    out, widest = pl.pallas_call(
        finish,
        out_shape=(
            jax.ShapeDtypeStruct((32, QGROUP), jnp.float32),
            jax.ShapeDtypeStruct((1, 32), jnp.float32),
        ),
        in_specs=[pl.BlockSpec(memory_space=pltpu.VMEM)] * 2,
        out_specs=[pl.BlockSpec(memory_space=pl.ANY)] * 2,
        scratch_shapes=[dma((2,))],
    )(
        pltpu.with_memory_space_constraint(turned, pltpu.VMEM),
        pltpu.with_memory_space_constraint(most, pltpu.VMEM),
    )
    return out.reshape(-1), widest.reshape(-1)


def solution(mesh):
    in_specs = (P("node", "local", None), P())
    out_specs = (P(("node", "local")), P(("node", "local")))
    return jax.shard_map(shards, mesh=mesh, in_specs=in_specs, out_specs=out_specs, check_vma=False)
```

```python
import functools

import jax
import jax.numpy as jnp
from jax import lax
from jax.experimental import pallas as pl
from jax.experimental.pallas import tpu as pltpu
from jax.sharding import PartitionSpec as P

ROT = 256
QGROUP = 128
MESH = pl.DeviceIdType.MESH
NEAR_LAST = (2, 1, 3, 0)
LOADS = ((0, 2), (2, 4), (4, 8), (8, 12), (12, 16), (16, 32))
PARTS = ((0, 0, 64), (0, 64, 64), (1, 0, 128))
FAR_FIRST = (6, 7, 4, 5, 2, 3, 1)


def power_below(values):
    lifted = values * 2.0**23
    nearest = (values + lifted) - lifted
    return jnp.where(nearest > values, 0.5 * nearest, nearest)


def encode(values):
    largest = jnp.max(jnp.abs(values), axis=0, keepdims=True)
    power = power_below(jnp.clip(largest, 2.0**-30, 1.5 * 2.0**30))
    inverse = 1.0 / power
    lifted = inverse * 2.0**23
    inverse = (inverse + lifted) - lifted
    units = jnp.trunc(values * (inverse * 2.0**17))
    anchor = jnp.maximum(jnp.abs(units) * 2.0**20, 1.5 * 2.0**24)
    code = (units * (1.0 + 2.0**-20) + anchor) - anchor
    return code * (power * 2.0**-17)


def kernel(
    x_hbm,
    signs_hbm,
    out_ref,
    max_ref,
    x_in,
    signs_in,
    own_signs,
    matrix,
    rows,
    coded,
    got_a,
    part,
    got_b,
    pair,
    got_c,
    recoded,
    got_n,
    told,
    in_sem,
    a_send,
    a_recv,
    b_send,
    b_recv,
    c_send,
    c_recv,
    n_send,
    n_recv,
):
    node, local = lax.axis_index("node"), lax.axis_index("local")
    me_y, me_x, me_z = local // 8, lax.rem(local // 2, 4), lax.rem(local, 2)

    def ahead(place, step):
        return lax.rem(place + step, 4)

    def device(y, x, z):
        return (node, y * 8 + x * 2 + z)

    def place_z(own):
        return me_z if own else 1 - me_z

    first_of = (me_x, me_y)
    second_of = (me_y, me_x)

    def along_first(h, step):
        if h == 0:
            return device(me_y, ahead(me_x, step), me_z)
        return device(ahead(me_y, step), me_x, me_z)

    def along_second(h, step):
        return along_first(1 - h, step)

    z_low, core = node // 2, lax.rem(node, 2)
    barrier = pltpu.get_barrier_semaphore()

    def here(zl, to_core, to_local):
        pl.semaphore_signal(
            barrier, inc=1, device_id=(2 * zl + to_core, to_local), device_id_type=MESH
        )

    for h in range(2):
        for step in range(1, 4):
            here(z_low, 0, along_first(h, step)[1])
    for step in range(1, 4):
        here(ahead(z_low, step), 1, local)
    here(z_low, 1, me_y * 8 + me_x * 2 + 1 - me_z)

    @pl.when(core == 1)
    def _():
        here(z_low, 0, local)

    def tell_other_core():
        pl.semaphore_signal(
            told, inc=1, device_id=(2 * z_low + 1 - core, local), device_id_type=MESH
        )

    def tile_of(own, dy, dx):
        return ahead(me_y, dy) * 8 + ahead(me_x, dx) * 2 + place_z(own)

    def slot_of(own, dy, dx):
        return 16 * own + 4 * NEAR_LAST.index(dy) + NEAR_LAST.index(dx)

    def start_loads(group):
        first, last = LOADS[group]
        for slot in range(first, last):
            own, dy, dx = slot // 16, NEAR_LAST[slot // 4 % 4], NEAR_LAST[slot % 4]
            t = tile_of(own, dy, dx)
            pltpu.make_async_copy(x_hbm.at[:, t], x_in.at[slot], in_sem.at[0, group]).start()
            pltpu.make_async_copy(
                signs_hbm.at[:, t], signs_in.at[slot], in_sem.at[1, group]
            ).start()

    def wait_loads(group):
        first, last = LOADS[group]
        for n, buffer in enumerate((x_in, signs_in)):
            whole = buffer.at[pl.ds(first, last - first)]
            pltpu.make_async_copy(whole, whole, in_sem.at[n, group]).wait()

    start_loads(0)
    own_copy = pltpu.make_async_copy(signs_hbm.at[node, local], own_signs, in_sem.at[0, len(LOADS)])
    own_copy.start()

    i = lax.broadcasted_iota(jnp.int32, (ROT, ROT), 0)
    j = lax.broadcasted_iota(jnp.int32, (ROT, ROT), 1)
    odd = lax.population_count(i & j) & 1
    matrix[...] = (1 - 2 * odd).astype(jnp.float32).astype(jnp.bfloat16)

    def rows_of(p):
        return pl.ds(PARTS[p][1], PARTS[p][2])

    def send_a(p, h, c, step):
        own = PARTS[p][0]
        return pltpu.make_async_remote_copy(
            src_ref=coded.at[h, own, c, ahead(first_of[h], step), rows_of(p)],
            dst_ref=got_a.at[h, own, c, step - 1, rows_of(p)],
            send_sem=a_send,
            recv_sem=a_recv.at[h, p, c],
            device_id=along_first(h, step),
            device_id_type=MESH,
        )

    def send_b(p, h, step):
        own = PARTS[p][0]
        return pltpu.make_async_remote_copy(
            src_ref=part.at[h, own, ahead(second_of[h], step), rows_of(p)],
            dst_ref=got_b.at[h, own, step - 1, rows_of(p)],
            send_sem=b_send,
            recv_sem=b_recv.at[h, p],
            device_id=along_second(h, step),
            device_id_type=MESH,
        )

    def send_c(p, h):
        return pltpu.make_async_remote_copy(
            src_ref=pair.at[h, rows_of(p)],
            dst_ref=got_c.at[h, rows_of(p)],
            send_sem=c_send,
            recv_sem=c_recv.at[h, p],
            device_id=device(me_y, me_x, 1 - me_z),
            device_id_type=MESH,
        )

    def send_n(h, k):
        z = z_low
        if k & 4:
            z = lax.rem(z + 2, 4)
        if k & 2:
            z = z + 1 - 2 * lax.rem(z, 2)
        to = 2 * z + (1 - core if k & 1 else core)
        return pltpu.make_async_remote_copy(
            src_ref=recoded.at[to, h],
            dst_ref=got_n.at[h, k - 1],
            send_sem=n_send,
            recv_sem=n_recv.at[h],
            device_id=(to, local),
            device_id_type=MESH,
        )

    def rotate(own, dy, steps):
        for k, dx in enumerate(steps):
            t = slot_of(own, dy, dx)
            for g in range(8):
                for q in range(4):
                    v = x_in[t, g, :, pl.ds(q * 1024, 1024)].astype(jnp.float32).reshape(8, 128)
                    s = signs_in[t, g, pl.ds(q * 8, 8), :]
                    rows[k, pl.ds(g * 32 + q * 8, 8), :] = jnp.where(s == 0, v, -v)
        for k, dx in enumerate(steps):
            blocks = jnp.concatenate(
                [
                    rows[k, pl.ds(0, 128, 2), :].astype(jnp.bfloat16),
                    rows[k, pl.ds(1, 128, 2), :].astype(jnp.bfloat16),
                ],
                axis=1,
            )
            rotated = lax.dot_general(
                matrix[...],
                blocks,
                (((1,), (1,)), ((), ())),
                preferred_element_type=jnp.float32,
            )
            y, x = ahead(me_y, dy), ahead(me_x, dx)
            coded[0, own, y, x] = encode(rotated[:QGROUP]).astype(jnp.bfloat16)
            coded[1, own, x, y] = encode(rotated[QGROUP:]).astype(jnp.bfloat16)

    def send_tiles(dy, steps):
        for dx in steps:
            if dx:
                send_a(0, 0, ahead(me_y, dy), dx).start()
            if dy:
                send_a(0, 1, ahead(me_x, dx), dy).start()

    def send_chunk(p, step):
        for to in NEAR_LAST[:3]:
            for h in range(2):
                send_a(p, h, ahead(second_of[h], step), to).start()

    def wait_for(buffer, sem):
        pltpu.make_async_copy(buffer, buffer, sem).wait()

    def reduce_first(p, step):
        own, rows = PARTS[p][0], rows_of(p)
        for h in range(2):
            c = ahead(second_of[h], step)
            wait_for(got_a.at[h, own, c, pl.ds(0, 3), rows], a_recv.at[h, p, c])
            total = coded[h, own, c, first_of[h], rows].astype(jnp.float32)
            for k in range(3):
                total += got_a[h, own, c, k, rows].astype(jnp.float32)
            part[h, own, c, rows] = total
            if step:
                send_b(p, h, step).start()

    def reduce_second(p, h):
        own, rows = PARTS[p][0], rows_of(p)
        wait_for(got_b.at[h, own, pl.ds(0, 3), rows], b_recv.at[h, p])
        total = part[h, own, second_of[h], rows]
        for k in range(3):
            total += got_b[h, own, k, rows]
        return total

    def exchange_z(p):
        for h in range(2):
            pair[h, rows_of(p)] = reduce_second(p, h)
            send_c(p, h).start()

    first_row, *other_rows = NEAR_LAST
    wait_loads(0)
    rotate(0, first_row, NEAR_LAST[:2])
    for group in range(1, len(LOADS)):
        start_loads(group)

    @pl.when(core == 0)
    def _():
        pl.semaphore_wait(barrier, 13)
        tell_other_core()

    @pl.when(core == 1)
    def _():
        pl.semaphore_wait(told, 1)

    send_tiles(first_row, NEAR_LAST[:2])
    wait_loads(1)
    rotate(0, first_row, NEAR_LAST[2:])
    send_tiles(first_row, NEAR_LAST[2:])
    for n, dy in enumerate(other_rows):
        wait_loads(2 + n)
        rotate(0, dy, NEAR_LAST)
        send_tiles(dy, NEAR_LAST)
    for step in NEAR_LAST:
        send_chunk(1, step)
    wait_loads(5)
    for dy in NEAR_LAST:
        rotate(1, dy, NEAR_LAST)
    for step in NEAR_LAST:
        reduce_first(0, step)
    send_chunk(2, 2)
    for step in NEAR_LAST:
        reduce_first(1, step)
    send_chunk(2, 1)

    @pl.when(core == 1)
    def _():
        pl.semaphore_wait(barrier, 8)
        tell_other_core()

    @pl.when(core == 0)
    def _():
        pl.semaphore_wait(told, 1)

    exchange_z(0)
    send_chunk(2, 3)
    send_chunk(2, 0)
    exchange_z(1)
    for step in NEAR_LAST:
        reduce_first(2, step)
    for h in range(2):
        first = reduce_second(2, h)
        wait_for(got_c.at[h, rows_of(0)], c_recv.at[h, 0])
        wait_for(got_c.at[h, rows_of(1)], c_recv.at[h, 1])
        decoded = encode(first + got_c[h])
        recoded[:, h] = decoded.T.astype(jnp.bfloat16).reshape(8, 16, QGROUP)
        for k in FAR_FIRST:
            send_n(h, k).start()
    own_copy.wait()
    wait_for(got_a, a_send)
    wait_for(got_b, b_send)
    wait_for(got_c, c_send)
    second = [recoded[node, h].astype(jnp.float32) for h in range(2)]
    for h in range(2):
        wait_for(got_n.at[h], n_recv.at[h])
        for k in reversed(FAR_FIRST):
            second[h] += got_n[h, k - 1].astype(jnp.float32)

    lane = lax.broadcasted_iota(jnp.int32, (16, 32), 1)
    block = lax.broadcasted_iota(jnp.int32, (16, 32), 0)
    widest = jnp.zeros((1, 32), jnp.float32)
    for h in range(2):
        most = jnp.max(jnp.abs(second[h]), axis=1, keepdims=True) * (1.0 / 16.0)
        widest += jnp.sum(jnp.where(lane == 2 * block + h, most, 0.0), axis=0, keepdims=True)
    max_ref[...] = widest

    whole = jnp.concatenate(second, axis=1)
    high = whole.astype(jnp.bfloat16)
    rest = whole - high.astype(jnp.float32)
    middle = rest.astype(jnp.bfloat16)
    low = (rest - middle.astype(jnp.float32)).astype(jnp.bfloat16)
    pieces = jnp.concatenate([high, middle, low], axis=0)
    back = jnp.dot(pieces, matrix[...], preferred_element_type=jnp.float32)
    back = ((back[32:48] + back[16:32]) + back[0:16]) * (1.0 / ROT)
    for h in range(2):
        s = own_signs[pl.ds(h, 16, 2), :]
        half = back[:, h * QGROUP : (h + 1) * QGROUP]
        out_ref[pl.ds(h, 16, 2), :] = jnp.where(s == 0, half, -half)

    wait_for(got_n, n_send)


def finish(turned_ref, most_ref, out_ref, max_ref, sem):
    copies = (
        pltpu.make_async_copy(turned_ref, out_ref, sem.at[0]),
        pltpu.make_async_copy(most_ref, max_ref, sem.at[1]),
    )
    for copy in copies:
        copy.start()
    for copy in copies:
        copy.wait()


def shards(partials, signs):
    dma = pltpu.SemaphoreType.DMA
    turned, most = pl.pallas_call(
        kernel,
        out_shape=(pltpu.VMEM((32, QGROUP), jnp.float32), pltpu.VMEM((1, 32), jnp.float32)),
        in_specs=[pl.BlockSpec(memory_space=pl.ANY)] * 2,
        out_specs=(
            pl.BlockSpec(memory_space=pltpu.VMEM),
            pl.BlockSpec(memory_space=pltpu.VMEM),
        ),
        scratch_shapes=[
            pltpu.VMEM((32, 8, 1, 4096), jnp.bfloat16),
            pltpu.VMEM((32, 8, 32, QGROUP), jnp.int32),
            pltpu.VMEM((32, QGROUP), jnp.int32),
            pltpu.VMEM((ROT, ROT), jnp.bfloat16),
            pltpu.VMEM((4, ROT, QGROUP), jnp.float32),
            pltpu.VMEM((2, 2, 4, 4, QGROUP, QGROUP), jnp.bfloat16),
            pltpu.VMEM((2, 2, 4, 3, QGROUP, QGROUP), jnp.bfloat16),
            pltpu.VMEM((2, 2, 4, QGROUP, QGROUP), jnp.float32),
            pltpu.VMEM((2, 2, 3, QGROUP, QGROUP), jnp.float32),
            pltpu.VMEM((2, QGROUP, QGROUP), jnp.float32),
            pltpu.VMEM((2, QGROUP, QGROUP), jnp.float32),
            pltpu.VMEM((8, 2, 16, QGROUP), jnp.bfloat16),
            pltpu.VMEM((2, 7, 16, QGROUP), jnp.bfloat16),
            pltpu.SemaphoreType.REGULAR,
            dma((2, len(LOADS) + 1)),
            dma,
            dma((2, 3, 4)),
            dma,
            dma((2, 3)),
            dma,
            dma((2, 2)),
            dma,
            dma((2,)),
        ],
        compiler_params=pltpu.CompilerParams(collective_id=0, has_side_effects=True),
    )(partials.reshape(8, 32, 1, 4096), signs.reshape(8, 32, 32, QGROUP))
    out, widest = pl.pallas_call(
        finish,
        out_shape=(
            jax.ShapeDtypeStruct((32, QGROUP), jnp.float32),
            jax.ShapeDtypeStruct((1, 32), jnp.float32),
        ),
        in_specs=[pl.BlockSpec(memory_space=pltpu.VMEM)] * 2,
        out_specs=[pl.BlockSpec(memory_space=pl.ANY)] * 2,
        scratch_shapes=[dma((2,))],
    )(
        pltpu.with_memory_space_constraint(turned, pltpu.VMEM),
        pltpu.with_memory_space_constraint(most, pltpu.VMEM),
    )
    return out.reshape(-1), widest.reshape(-1)


def solution(mesh):
    in_specs = (P("node", "local", None), P())
    out_specs = (P(("node", "local")), P(("node", "local")))
    return jax.shard_map(shards, mesh=mesh, in_specs=in_specs, out_specs=out_specs, check_vma=False)
```

```python
import functools

import jax
import jax.numpy as jnp
from jax import lax
from jax.experimental import pallas as pl
from jax.experimental.pallas import tpu as pltpu
from jax.sharding import PartitionSpec as P

ROT = 256
QGROUP = 128
MESH = pl.DeviceIdType.MESH
NEAR_LAST = (2, 1, 3, 0)
LOADS = ((0, 2), (2, 4), (4, 8), (8, 12), (12, 16), (16, 32))
PARTS = ((0, 0, 64), (0, 64, 64), (1, 0, 128))
FAR_FIRST = (6, 7, 4, 5, 2, 3, 1)


def power_below(values):
    lifted = values * 2.0**23
    nearest = (values + lifted) - lifted
    return jnp.where(nearest > values, 0.5 * nearest, nearest)


def encode(values):
    largest = jnp.max(jnp.abs(values), axis=0, keepdims=True)
    power = power_below(jnp.clip(largest, 2.0**-30, 1.5 * 2.0**30))
    inverse = 1.0 / power
    lifted = inverse * 2.0**23
    inverse = (inverse + lifted) - lifted
    units = jnp.trunc(values * (inverse * 2.0**17))
    anchor = jnp.maximum(jnp.abs(units) * 2.0**20, 1.5 * 2.0**24)
    code = (units * (1.0 + 2.0**-20) + anchor) - anchor
    return code * (power * 2.0**-17)


def kernel(
    x_hbm,
    signs_hbm,
    out_ref,
    max_ref,
    x_in,
    signs_in,
    own_signs,
    matrix,
    rows,
    coded,
    got_a,
    part,
    got_b,
    pair,
    got_c,
    recoded,
    got_n,
    told,
    in_sem,
    a_send,
    a_recv,
    b_send,
    b_recv,
    c_send,
    c_recv,
    n_send,
    n_recv,
):
    node, local = lax.axis_index("node"), lax.axis_index("local")
    me_y, me_x, me_z = local // 8, lax.rem(local // 2, 4), lax.rem(local, 2)

    def ahead(place, step):
        return lax.rem(place + step, 4)

    def device(y, x, z):
        return (node, y * 8 + x * 2 + z)

    def place_z(own):
        return me_z if own else 1 - me_z

    first_of = (me_x, me_y)
    second_of = (me_y, me_x)

    def along_first(h, step):
        if h == 0:
            return device(me_y, ahead(me_x, step), me_z)
        return device(ahead(me_y, step), me_x, me_z)

    def along_second(h, step):
        return along_first(1 - h, step)

    z_low, core = node // 2, lax.rem(node, 2)
    barrier = pltpu.get_barrier_semaphore()

    def here(zl, to_core, to_local):
        pl.semaphore_signal(
            barrier, inc=1, device_id=(2 * zl + to_core, to_local), device_id_type=MESH
        )

    for h in range(2):
        for step in range(1, 4):
            here(z_low, 0, along_first(h, step)[1])
    for step in range(1, 4):
        here(ahead(z_low, step), 1, local)
    here(z_low, 1, me_y * 8 + me_x * 2 + 1 - me_z)

    @pl.when(core == 1)
    def _():
        here(z_low, 0, local)

    def tell_other_core():
        pl.semaphore_signal(
            told, inc=1, device_id=(2 * z_low + 1 - core, local), device_id_type=MESH
        )

    def tile_of(own, dy, dx):
        return ahead(me_y, dy) * 8 + ahead(me_x, dx) * 2 + place_z(own)

    def slot_of(own, dy, dx):
        return 16 * own + 4 * NEAR_LAST.index(dy) + NEAR_LAST.index(dx)

    def start_loads(group):
        first, last = LOADS[group]
        for slot in range(first, last):
            own, dy, dx = slot // 16, NEAR_LAST[slot // 4 % 4], NEAR_LAST[slot % 4]
            t = tile_of(own, dy, dx)
            pltpu.make_async_copy(x_hbm.at[:, t], x_in.at[slot], in_sem.at[0, group]).start()
            pltpu.make_async_copy(
                signs_hbm.at[:, t], signs_in.at[slot], in_sem.at[1, group]
            ).start()

    def wait_loads(group):
        first, last = LOADS[group]
        for n, buffer in enumerate((x_in, signs_in)):
            whole = buffer.at[pl.ds(first, last - first)]
            pltpu.make_async_copy(whole, whole, in_sem.at[n, group]).wait()

    start_loads(0)
    own_copy = pltpu.make_async_copy(signs_hbm.at[node, local], own_signs, in_sem.at[0, len(LOADS)])
    own_copy.start()

    i = lax.broadcasted_iota(jnp.int32, (ROT, ROT), 0)
    j = lax.broadcasted_iota(jnp.int32, (ROT, ROT), 1)
    odd = lax.population_count(i & j) & 1
    matrix[...] = (1 - 2 * odd).astype(jnp.float32).astype(jnp.bfloat16)

    def rows_of(p):
        return pl.ds(PARTS[p][1], PARTS[p][2])

    def send_a(p, h, c, step):
        own = PARTS[p][0]
        return pltpu.make_async_remote_copy(
            src_ref=coded.at[h, own, c, ahead(first_of[h], step), rows_of(p)],
            dst_ref=got_a.at[h, own, c, step - 1, rows_of(p)],
            send_sem=a_send,
            recv_sem=a_recv.at[h, p, c],
            device_id=along_first(h, step),
            device_id_type=MESH,
        )

    def send_b(p, h, step):
        own = PARTS[p][0]
        return pltpu.make_async_remote_copy(
            src_ref=part.at[h, own, ahead(second_of[h], step), rows_of(p)],
            dst_ref=got_b.at[h, own, step - 1, rows_of(p)],
            send_sem=b_send,
            recv_sem=b_recv.at[h, p],
            device_id=along_second(h, step),
            device_id_type=MESH,
        )

    def send_c(p, h):
        return pltpu.make_async_remote_copy(
            src_ref=pair.at[h, rows_of(p)],
            dst_ref=got_c.at[h, rows_of(p)],
            send_sem=c_send,
            recv_sem=c_recv.at[h, p],
            device_id=device(me_y, me_x, 1 - me_z),
            device_id_type=MESH,
        )

    def send_n(h, k):
        z = z_low
        if k & 4:
            z = lax.rem(z + 2, 4)
        if k & 2:
            z = z + 1 - 2 * lax.rem(z, 2)
        to = 2 * z + (1 - core if k & 1 else core)
        return pltpu.make_async_remote_copy(
            src_ref=recoded.at[to, h],
            dst_ref=got_n.at[h, k - 1],
            send_sem=n_send,
            recv_sem=n_recv.at[h],
            device_id=(to, local),
            device_id_type=MESH,
        )

    def rotate(own, dy, steps):
        for k, dx in enumerate(steps):
            t = slot_of(own, dy, dx)
            for g in range(8):
                for q in range(4):
                    v = x_in[t, g, :, pl.ds(q * 1024, 1024)].astype(jnp.float32).reshape(8, 128)
                    s = signs_in[t, g, pl.ds(q * 8, 8), :]
                    rows[k, pl.ds(g * 32 + q * 8, 8), :] = jnp.where(s == 0, v, -v)
        for k, dx in enumerate(steps):
            blocks = jnp.concatenate(
                [
                    rows[k, pl.ds(0, 128, 2), :].astype(jnp.bfloat16),
                    rows[k, pl.ds(1, 128, 2), :].astype(jnp.bfloat16),
                ],
                axis=1,
            )
            rotated = lax.dot_general(
                matrix[...],
                blocks,
                (((1,), (1,)), ((), ())),
                preferred_element_type=jnp.float32,
            )
            y, x = ahead(me_y, dy), ahead(me_x, dx)
            coded[0, own, y, x] = encode(rotated[:QGROUP]).astype(jnp.bfloat16)
            coded[1, own, x, y] = encode(rotated[QGROUP:]).astype(jnp.bfloat16)

    def send_tiles(dy, steps):
        for dx in steps:
            if dx:
                send_a(0, 0, ahead(me_y, dy), dx).start()
            if dy:
                send_a(0, 1, ahead(me_x, dx), dy).start()

    def send_chunk(p, step):
        for to in NEAR_LAST[:3]:
            for h in range(2):
                send_a(p, h, ahead(second_of[h], step), to).start()

    def wait_for(buffer, sem):
        pltpu.make_async_copy(buffer, buffer, sem).wait()

    def send_near(side, *steps):
        @pl.when(me_z == side)
        def _():
            for step in steps:
                send_chunk(2, step)

    def reduce_first(p, step):
        own, rows = PARTS[p][0], rows_of(p)
        for h in range(2):
            c = ahead(second_of[h], step)
            wait_for(got_a.at[h, own, c, pl.ds(0, 3), rows], a_recv.at[h, p, c])
            total = coded[h, own, c, first_of[h], rows].astype(jnp.float32)
            for k in range(3):
                total += got_a[h, own, c, k, rows].astype(jnp.float32)
            part[h, own, c, rows] = total
            if step:
                send_b(p, h, step).start()

    def reduce_second(p, h):
        own, rows = PARTS[p][0], rows_of(p)
        wait_for(got_b.at[h, own, pl.ds(0, 3), rows], b_recv.at[h, p])
        total = part[h, own, second_of[h], rows]
        for k in range(3):
            total += got_b[h, own, k, rows]
        return total

    def exchange_z(p):
        for h in range(2):
            pair[h, rows_of(p)] = reduce_second(p, h)
            send_c(p, h).start()

    first_row, *other_rows = NEAR_LAST
    wait_loads(0)
    rotate(0, first_row, NEAR_LAST[:2])
    for group in range(1, len(LOADS)):
        start_loads(group)

    @pl.when(core == 0)
    def _():
        pl.semaphore_wait(barrier, 13)
        tell_other_core()

    @pl.when(core == 1)
    def _():
        pl.semaphore_wait(told, 1)

    send_tiles(first_row, NEAR_LAST[:2])
    wait_loads(1)
    rotate(0, first_row, NEAR_LAST[2:])
    send_tiles(first_row, NEAR_LAST[2:])
    for n, dy in enumerate(other_rows):
        wait_loads(2 + n)
        rotate(0, dy, NEAR_LAST)
        send_tiles(dy, NEAR_LAST)
    for step in NEAR_LAST:
        send_chunk(1, step)
    wait_loads(5)
    for dy in NEAR_LAST:
        rotate(1, dy, NEAR_LAST)
    for step in NEAR_LAST:
        reduce_first(0, step)
    send_near(0, 2)
    for step in NEAR_LAST:
        reduce_first(1, step)
    send_near(0, 1)

    @pl.when(core == 1)
    def _():
        pl.semaphore_wait(barrier, 8)
        tell_other_core()

    @pl.when(core == 0)
    def _():
        pl.semaphore_wait(told, 1)

    exchange_z(0)
    send_near(0, 3, 0)
    send_near(1, 2)
    exchange_z(1)
    send_near(1, 1, 3, 0)
    for step in NEAR_LAST:
        reduce_first(2, step)
    for h in range(2):
        first = reduce_second(2, h)
        wait_for(got_c.at[h, rows_of(0)], c_recv.at[h, 0])
        wait_for(got_c.at[h, rows_of(1)], c_recv.at[h, 1])
        decoded = encode(first + got_c[h])
        recoded[:, h] = decoded.T.astype(jnp.bfloat16).reshape(8, 16, QGROUP)
        for k in FAR_FIRST:
            send_n(h, k).start()
    own_copy.wait()
    wait_for(got_a, a_send)
    wait_for(got_b, b_send)
    wait_for(got_c, c_send)
    second = [recoded[node, h].astype(jnp.float32) for h in range(2)]
    for h in range(2):
        wait_for(got_n.at[h], n_recv.at[h])
        for k in reversed(FAR_FIRST):
            second[h] += got_n[h, k - 1].astype(jnp.float32)

    lane = lax.broadcasted_iota(jnp.int32, (16, 32), 1)
    block = lax.broadcasted_iota(jnp.int32, (16, 32), 0)
    widest = jnp.zeros((1, 32), jnp.float32)
    for h in range(2):
        most = jnp.max(jnp.abs(second[h]), axis=1, keepdims=True) * (1.0 / 16.0)
        widest += jnp.sum(jnp.where(lane == 2 * block + h, most, 0.0), axis=0, keepdims=True)
    max_ref[...] = widest

    whole = jnp.concatenate(second, axis=1)
    high = whole.astype(jnp.bfloat16)
    rest = whole - high.astype(jnp.float32)
    middle = rest.astype(jnp.bfloat16)
    low = (rest - middle.astype(jnp.float32)).astype(jnp.bfloat16)
    pieces = jnp.concatenate([high, middle, low], axis=0)
    back = jnp.dot(pieces, matrix[...], preferred_element_type=jnp.float32)
    back = ((back[32:48] + back[16:32]) + back[0:16]) * (1.0 / ROT)
    for h in range(2):
        s = own_signs[pl.ds(h, 16, 2), :]
        half = back[:, h * QGROUP : (h + 1) * QGROUP]
        out_ref[pl.ds(h, 16, 2), :] = jnp.where(s == 0, half, -half)

    wait_for(got_n, n_send)


def finish(turned_ref, most_ref, out_ref, max_ref, sem):
    copies = (
        pltpu.make_async_copy(turned_ref, out_ref, sem.at[0]),
        pltpu.make_async_copy(most_ref, max_ref, sem.at[1]),
    )
    for copy in copies:
        copy.start()
    for copy in copies:
        copy.wait()


def shards(partials, signs):
    dma = pltpu.SemaphoreType.DMA
    turned, most = pl.pallas_call(
        kernel,
        out_shape=(pltpu.VMEM((32, QGROUP), jnp.float32), pltpu.VMEM((1, 32), jnp.float32)),
        in_specs=[pl.BlockSpec(memory_space=pl.ANY)] * 2,
        out_specs=(
            pl.BlockSpec(memory_space=pltpu.VMEM),
            pl.BlockSpec(memory_space=pltpu.VMEM),
        ),
        scratch_shapes=[
            pltpu.VMEM((32, 8, 1, 4096), jnp.bfloat16),
            pltpu.VMEM((32, 8, 32, QGROUP), jnp.int32),
            pltpu.VMEM((32, QGROUP), jnp.int32),
            pltpu.VMEM((ROT, ROT), jnp.bfloat16),
            pltpu.VMEM((4, ROT, QGROUP), jnp.float32),
            pltpu.VMEM((2, 2, 4, 4, QGROUP, QGROUP), jnp.bfloat16),
            pltpu.VMEM((2, 2, 4, 3, QGROUP, QGROUP), jnp.bfloat16),
            pltpu.VMEM((2, 2, 4, QGROUP, QGROUP), jnp.float32),
            pltpu.VMEM((2, 2, 3, QGROUP, QGROUP), jnp.float32),
            pltpu.VMEM((2, QGROUP, QGROUP), jnp.float32),
            pltpu.VMEM((2, QGROUP, QGROUP), jnp.float32),
            pltpu.VMEM((8, 2, 16, QGROUP), jnp.bfloat16),
            pltpu.VMEM((2, 7, 16, QGROUP), jnp.bfloat16),
            pltpu.SemaphoreType.REGULAR,
            dma((2, len(LOADS) + 1)),
            dma,
            dma((2, 3, 4)),
            dma,
            dma((2, 3)),
            dma,
            dma((2, 2)),
            dma,
            dma((2,)),
        ],
        compiler_params=pltpu.CompilerParams(collective_id=0, has_side_effects=True),
    )(partials.reshape(8, 32, 1, 4096), signs.reshape(8, 32, 32, QGROUP))
    out, widest = pl.pallas_call(
        finish,
        out_shape=(
            jax.ShapeDtypeStruct((32, QGROUP), jnp.float32),
            jax.ShapeDtypeStruct((1, 32), jnp.float32),
        ),
        in_specs=[pl.BlockSpec(memory_space=pltpu.VMEM)] * 2,
        out_specs=[pl.BlockSpec(memory_space=pl.ANY)] * 2,
        scratch_shapes=[dma((2,))],
    )(
        pltpu.with_memory_space_constraint(turned, pltpu.VMEM),
        pltpu.with_memory_space_constraint(most, pltpu.VMEM),
    )
    return out.reshape(-1), widest.reshape(-1)


def solution(mesh):
    in_specs = (P("node", "local", None), P())
    out_specs = (P(("node", "local")), P(("node", "local")))
    return jax.shard_map(shards, mesh=mesh, in_specs=in_specs, out_specs=out_specs, check_vma=False)
```

```python
import functools

import jax
import jax.numpy as jnp
from jax import lax
from jax.experimental import pallas as pl
from jax.experimental.pallas import tpu as pltpu
from jax.sharding import PartitionSpec as P

ROT = 256
QGROUP = 128
MESH = pl.DeviceIdType.MESH
NEAR_LAST = (2, 1, 3, 0)
LOADS = ((0, 2), (2, 4), (4, 8), (8, 12), (12, 16), (16, 32))
PARTS = ((0, 0, 64), (0, 64, 64), (1, 0, 128))
FAR_FIRST = (6, 7, 4, 5, 2, 3, 1)


def power_below(values):
    lifted = values * 2.0**23
    nearest = (values + lifted) - lifted
    return jnp.where(nearest > values, 0.5 * nearest, nearest)


def encode(values):
    largest = jnp.max(jnp.abs(values), axis=0, keepdims=True)
    power = power_below(jnp.clip(largest, 2.0**-30, 1.5 * 2.0**30))
    inverse = 1.0 / power
    lifted = inverse * 2.0**23
    inverse = (inverse + lifted) - lifted
    units = jnp.trunc(values * (inverse * 2.0**17))
    anchor = jnp.maximum(jnp.abs(units) * 2.0**20, 1.5 * 2.0**24)
    code = (units * (1.0 + 2.0**-20) + anchor) - anchor
    return code * (power * 2.0**-17)


def kernel(
    x_hbm,
    signs_hbm,
    out_ref,
    max_ref,
    x_in,
    signs_in,
    own_signs,
    matrix,
    rows,
    coded,
    got_a,
    part,
    got_b,
    pair,
    got_c,
    recoded,
    got_n,
    told,
    in_sem,
    a_send,
    a_recv,
    b_send,
    b_recv,
    c_send,
    c_recv,
    n_send,
    n_recv,
):
    node, local = lax.axis_index("node"), lax.axis_index("local")
    me_y, me_x, me_z = local // 8, lax.rem(local // 2, 4), lax.rem(local, 2)

    def ahead(place, step):
        return lax.rem(place + step, 4)

    def device(y, x, z):
        return (node, y * 8 + x * 2 + z)

    def place_z(own):
        return me_z if own else 1 - me_z

    first_of = (me_x, me_y)
    second_of = (me_y, me_x)

    def along_first(h, step):
        if h == 0:
            return device(me_y, ahead(me_x, step), me_z)
        return device(ahead(me_y, step), me_x, me_z)

    def along_second(h, step):
        return along_first(1 - h, step)

    z_low, core = node // 2, lax.rem(node, 2)
    barrier = pltpu.get_barrier_semaphore()

    def here(zl, to_core, to_local):
        pl.semaphore_signal(
            barrier, inc=1, device_id=(2 * zl + to_core, to_local), device_id_type=MESH
        )

    for h in range(2):
        for step in range(1, 4):
            here(z_low, 1, along_first(h, step)[1])
    for step in range(1, 4):
        here(ahead(z_low, step), 0, local)
    here(z_low, 0, me_y * 8 + me_x * 2 + 1 - me_z)

    @pl.when(core == 0)
    def _():
        here(z_low, 1, local)

    def tell_other_core():
        pl.semaphore_signal(
            told, inc=1, device_id=(2 * z_low + 1 - core, local), device_id_type=MESH
        )

    def tile_of(own, dy, dx):
        return ahead(me_y, dy) * 8 + ahead(me_x, dx) * 2 + place_z(own)

    def slot_of(own, dy, dx):
        return 16 * own + 4 * NEAR_LAST.index(dy) + NEAR_LAST.index(dx)

    def start_loads(group):
        first, last = LOADS[group]
        for slot in range(first, last):
            own, dy, dx = slot // 16, NEAR_LAST[slot // 4 % 4], NEAR_LAST[slot % 4]
            t = tile_of(own, dy, dx)
            pltpu.make_async_copy(x_hbm.at[:, t], x_in.at[slot], in_sem.at[0, group]).start()
            pltpu.make_async_copy(
                signs_hbm.at[:, t], signs_in.at[slot], in_sem.at[1, group]
            ).start()

    def wait_loads(group):
        first, last = LOADS[group]
        for n, buffer in enumerate((x_in, signs_in)):
            whole = buffer.at[pl.ds(first, last - first)]
            pltpu.make_async_copy(whole, whole, in_sem.at[n, group]).wait()

    start_loads(0)
    own_copy = pltpu.make_async_copy(signs_hbm.at[node, local], own_signs, in_sem.at[0, len(LOADS)])
    own_copy.start()

    i = lax.broadcasted_iota(jnp.int32, (ROT, ROT), 0)
    j = lax.broadcasted_iota(jnp.int32, (ROT, ROT), 1)
    odd = lax.population_count(i & j) & 1
    matrix[...] = (1 - 2 * odd).astype(jnp.float32).astype(jnp.bfloat16)

    def rows_of(p):
        return pl.ds(PARTS[p][1], PARTS[p][2])

    def send_a(p, h, c, step):
        own = PARTS[p][0]
        return pltpu.make_async_remote_copy(
            src_ref=coded.at[h, own, c, ahead(first_of[h], step), rows_of(p)],
            dst_ref=got_a.at[h, own, c, step - 1, rows_of(p)],
            send_sem=a_send,
            recv_sem=a_recv.at[h, p, c],
            device_id=along_first(h, step),
            device_id_type=MESH,
        )

    def send_b(p, h, step):
        own = PARTS[p][0]
        return pltpu.make_async_remote_copy(
            src_ref=part.at[h, own, ahead(second_of[h], step), rows_of(p)],
            dst_ref=got_b.at[h, own, step - 1, rows_of(p)],
            send_sem=b_send,
            recv_sem=b_recv.at[h, p],
            device_id=along_second(h, step),
            device_id_type=MESH,
        )

    def send_c(p, h):
        return pltpu.make_async_remote_copy(
            src_ref=pair.at[h, rows_of(p)],
            dst_ref=got_c.at[h, rows_of(p)],
            send_sem=c_send,
            recv_sem=c_recv.at[h, p],
            device_id=device(me_y, me_x, 1 - me_z),
            device_id_type=MESH,
        )

    def send_n(h, k):
        z = z_low
        if k & 4:
            z = lax.rem(z + 2, 4)
        if k & 2:
            z = z + 1 - 2 * lax.rem(z, 2)
        to = 2 * z + (1 - core if k & 1 else core)
        return pltpu.make_async_remote_copy(
            src_ref=recoded.at[to, h],
            dst_ref=got_n.at[h, k - 1],
            send_sem=n_send,
            recv_sem=n_recv.at[h],
            device_id=(to, local),
            device_id_type=MESH,
        )

    def rotate(own, dy, steps):
        for k, dx in enumerate(steps):
            t = slot_of(own, dy, dx)
            for g in range(8):
                for q in range(4):
                    v = x_in[t, g, :, pl.ds(q * 1024, 1024)].astype(jnp.float32).reshape(8, 128)
                    s = signs_in[t, g, pl.ds(q * 8, 8), :]
                    rows[k, pl.ds(g * 32 + q * 8, 8), :] = jnp.where(s == 0, v, -v)
        for k, dx in enumerate(steps):
            blocks = jnp.concatenate(
                [
                    rows[k, pl.ds(0, 128, 2), :].astype(jnp.bfloat16),
                    rows[k, pl.ds(1, 128, 2), :].astype(jnp.bfloat16),
                ],
                axis=1,
            )
            rotated = lax.dot_general(
                matrix[...],
                blocks,
                (((1,), (1,)), ((), ())),
                preferred_element_type=jnp.float32,
            )
            y, x = ahead(me_y, dy), ahead(me_x, dx)
            coded[0, own, y, x] = encode(rotated[:QGROUP]).astype(jnp.bfloat16)
            coded[1, own, x, y] = encode(rotated[QGROUP:]).astype(jnp.bfloat16)

    def send_tiles(dy, steps):
        for dx in steps:
            if dx:
                send_a(0, 0, ahead(me_y, dy), dx).start()
            if dy:
                send_a(0, 1, ahead(me_x, dx), dy).start()

    def send_chunk(p, step):
        for to in NEAR_LAST[:3]:
            for h in range(2):
                send_a(p, h, ahead(second_of[h], step), to).start()

    def wait_for(buffer, sem):
        pltpu.make_async_copy(buffer, buffer, sem).wait()

    def send_near(side, *steps):
        @pl.when(me_z == side)
        def _():
            for step in steps:
                send_chunk(2, step)

    def reduce_first(p, step):
        own, rows = PARTS[p][0], rows_of(p)
        for h in range(2):
            c = ahead(second_of[h], step)
            wait_for(got_a.at[h, own, c, pl.ds(0, 3), rows], a_recv.at[h, p, c])
            total = coded[h, own, c, first_of[h], rows].astype(jnp.float32)
            for k in range(3):
                total += got_a[h, own, c, k, rows].astype(jnp.float32)
            part[h, own, c, rows] = total
            if step:
                send_b(p, h, step).start()

    def reduce_second(p, h):
        own, rows = PARTS[p][0], rows_of(p)
        wait_for(got_b.at[h, own, pl.ds(0, 3), rows], b_recv.at[h, p])
        total = part[h, own, second_of[h], rows]
        for k in range(3):
            total += got_b[h, own, k, rows]
        return total

    def exchange_z(p):
        for h in range(2):
            pair[h, rows_of(p)] = reduce_second(p, h)
            send_c(p, h).start()

    first_row, *other_rows = NEAR_LAST
    wait_loads(0)
    rotate(0, first_row, NEAR_LAST[:2])
    for group in range(1, len(LOADS)):
        start_loads(group)

    @pl.when(core == 1)
    def _():
        pl.semaphore_wait(barrier, 13)
        tell_other_core()

    @pl.when(core == 0)
    def _():
        pl.semaphore_wait(told, 1)

    send_tiles(first_row, NEAR_LAST[:2])
    wait_loads(1)
    rotate(0, first_row, NEAR_LAST[2:])
    send_tiles(first_row, NEAR_LAST[2:])
    for n, dy in enumerate(other_rows):
        wait_loads(2 + n)
        rotate(0, dy, NEAR_LAST)
        send_tiles(dy, NEAR_LAST)
    for step in NEAR_LAST:
        send_chunk(1, step)
    wait_loads(5)
    for dy in NEAR_LAST:
        rotate(1, dy, NEAR_LAST)
    for step in NEAR_LAST:
        reduce_first(0, step)
    send_near(0, 2)
    for step in NEAR_LAST:
        reduce_first(1, step)
    send_near(0, 1)

    @pl.when(core == 0)
    def _():
        pl.semaphore_wait(barrier, 8)
        tell_other_core()

    @pl.when(core == 1)
    def _():
        pl.semaphore_wait(told, 1)

    exchange_z(0)
    send_near(0, 3, 0)
    exchange_z(1)
    send_near(1, 2, 1, 3, 0)
    for step in NEAR_LAST:
        reduce_first(2, step)
    for h in range(2):
        first = reduce_second(2, h)
        wait_for(got_c.at[h, rows_of(0)], c_recv.at[h, 0])
        wait_for(got_c.at[h, rows_of(1)], c_recv.at[h, 1])
        decoded = encode(first + got_c[h])
        recoded[:, h] = decoded.T.astype(jnp.bfloat16).reshape(8, 16, QGROUP)
        for k in FAR_FIRST:
            send_n(h, k).start()
    own_copy.wait()
    wait_for(got_a, a_send)
    wait_for(got_b, b_send)
    wait_for(got_c, c_send)
    second = [recoded[node, h].astype(jnp.float32) for h in range(2)]
    for h in range(2):
        wait_for(got_n.at[h], n_recv.at[h])
        for k in reversed(FAR_FIRST):
            second[h] += got_n[h, k - 1].astype(jnp.float32)

    lane = lax.broadcasted_iota(jnp.int32, (16, 32), 1)
    block = lax.broadcasted_iota(jnp.int32, (16, 32), 0)
    widest = jnp.zeros((1, 32), jnp.float32)
    for h in range(2):
        most = jnp.max(jnp.abs(second[h]), axis=1, keepdims=True) * (1.0 / 16.0)
        widest += jnp.sum(jnp.where(lane == 2 * block + h, most, 0.0), axis=0, keepdims=True)
    max_ref[...] = widest

    whole = jnp.concatenate(second, axis=1)
    high = whole.astype(jnp.bfloat16)
    rest = whole - high.astype(jnp.float32)
    middle = rest.astype(jnp.bfloat16)
    low = (rest - middle.astype(jnp.float32)).astype(jnp.bfloat16)
    pieces = jnp.concatenate([high, middle, low], axis=0)
    back = jnp.dot(pieces, matrix[...], preferred_element_type=jnp.float32)
    back = ((back[32:48] + back[16:32]) + back[0:16]) * (1.0 / ROT)
    for h in range(2):
        s = own_signs[pl.ds(h, 16, 2), :]
        half = back[:, h * QGROUP : (h + 1) * QGROUP]
        out_ref[pl.ds(h, 16, 2), :] = jnp.where(s == 0, half, -half)

    wait_for(got_n, n_send)


def finish(turned_ref, most_ref, out_ref, max_ref, sem):
    copies = (
        pltpu.make_async_copy(turned_ref, out_ref, sem.at[0]),
        pltpu.make_async_copy(most_ref, max_ref, sem.at[1]),
    )
    for copy in copies:
        copy.start()
    for copy in copies:
        copy.wait()


def shards(partials, signs):
    dma = pltpu.SemaphoreType.DMA
    turned, most = pl.pallas_call(
        kernel,
        out_shape=(pltpu.VMEM((32, QGROUP), jnp.float32), pltpu.VMEM((1, 32), jnp.float32)),
        in_specs=[pl.BlockSpec(memory_space=pl.ANY)] * 2,
        out_specs=(
            pl.BlockSpec(memory_space=pltpu.VMEM),
            pl.BlockSpec(memory_space=pltpu.VMEM),
        ),
        scratch_shapes=[
            pltpu.VMEM((32, 8, 1, 4096), jnp.bfloat16),
            pltpu.VMEM((32, 8, 32, QGROUP), jnp.int32),
            pltpu.VMEM((32, QGROUP), jnp.int32),
            pltpu.VMEM((ROT, ROT), jnp.bfloat16),
            pltpu.VMEM((4, ROT, QGROUP), jnp.float32),
            pltpu.VMEM((2, 2, 4, 4, QGROUP, QGROUP), jnp.bfloat16),
            pltpu.VMEM((2, 2, 4, 3, QGROUP, QGROUP), jnp.bfloat16),
            pltpu.VMEM((2, 2, 4, QGROUP, QGROUP), jnp.float32),
            pltpu.VMEM((2, 2, 3, QGROUP, QGROUP), jnp.float32),
            pltpu.VMEM((2, QGROUP, QGROUP), jnp.float32),
            pltpu.VMEM((2, QGROUP, QGROUP), jnp.float32),
            pltpu.VMEM((8, 2, 16, QGROUP), jnp.bfloat16),
            pltpu.VMEM((2, 7, 16, QGROUP), jnp.bfloat16),
            pltpu.SemaphoreType.REGULAR,
            dma((2, len(LOADS) + 1)),
            dma,
            dma((2, 3, 4)),
            dma,
            dma((2, 3)),
            dma,
            dma((2, 2)),
            dma,
            dma((2,)),
        ],
        compiler_params=pltpu.CompilerParams(collective_id=0, has_side_effects=True),
    )(partials.reshape(8, 32, 1, 4096), signs.reshape(8, 32, 32, QGROUP))
    out, widest = pl.pallas_call(
        finish,
        out_shape=(
            jax.ShapeDtypeStruct((32, QGROUP), jnp.float32),
            jax.ShapeDtypeStruct((1, 32), jnp.float32),
        ),
        in_specs=[pl.BlockSpec(memory_space=pltpu.VMEM)] * 2,
        out_specs=[pl.BlockSpec(memory_space=pl.ANY)] * 2,
        scratch_shapes=[dma((2,))],
    )(
        pltpu.with_memory_space_constraint(turned, pltpu.VMEM),
        pltpu.with_memory_space_constraint(most, pltpu.VMEM),
    )
    return out.reshape(-1), widest.reshape(-1)


def solution(mesh):
    in_specs = (P("node", "local", None), P())
    out_specs = (P(("node", "local")), P(("node", "local")))
    return jax.shard_map(shards, mesh=mesh, in_specs=in_specs, out_specs=out_specs, check_vma=False)
```

```python
import functools

import jax
import jax.numpy as jnp
from jax import lax
from jax.experimental import pallas as pl
from jax.experimental.pallas import tpu as pltpu
from jax.sharding import PartitionSpec as P

ROT = 256
QGROUP = 128
MESH = pl.DeviceIdType.MESH
NEAR_LAST = (2, 1, 3, 0)
LOADS = ((0, 2), (2, 4), (4, 8), (8, 12), (12, 16), (16, 32))
PARTS = ((0, 0, 64), (0, 64, 64), (1, 0, 128))
FAR_FIRST = (6, 7, 4, 5, 2, 3, 1)


def power_below(values):
    lifted = values * 2.0**23
    nearest = (values + lifted) - lifted
    return jnp.where(nearest > values, 0.5 * nearest, nearest)


def encode(values):
    largest = jnp.max(jnp.abs(values), axis=0, keepdims=True)
    power = power_below(jnp.clip(largest, 2.0**-30, 1.5 * 2.0**30))
    inverse = 1.0 / power
    lifted = inverse * 2.0**23
    inverse = (inverse + lifted) - lifted
    units = jnp.trunc(values * (inverse * 2.0**17))
    anchor = jnp.maximum(jnp.abs(units) * 2.0**20, 1.5 * 2.0**24)
    code = (units * (1.0 + 2.0**-20) + anchor) - anchor
    return code * (power * 2.0**-17)


def kernel(
    x_hbm,
    signs_hbm,
    out_ref,
    max_ref,
    x_in,
    signs_in,
    own_signs,
    matrix,
    rows,
    coded,
    got_a,
    part,
    got_b,
    pair,
    got_c,
    recoded,
    got_n,
    told,
    in_sem,
    a_send,
    a_recv,
    b_send,
    b_recv,
    c_send,
    c_recv,
    n_send,
    n_recv,
):
    node, local = lax.axis_index("node"), lax.axis_index("local")
    me_y, me_x, me_z = local // 8, lax.rem(local // 2, 4), lax.rem(local, 2)

    def ahead(place, step):
        return lax.rem(place + step, 4)

    def device(y, x, z):
        return (node, y * 8 + x * 2 + z)

    def place_z(own):
        return me_z if own else 1 - me_z

    first_of = (me_x, me_y)
    second_of = (me_y, me_x)

    def along_first(h, step):
        if h == 0:
            return device(me_y, ahead(me_x, step), me_z)
        return device(ahead(me_y, step), me_x, me_z)

    def along_second(h, step):
        return along_first(1 - h, step)

    z_low, core = node // 2, lax.rem(node, 2)
    barrier = pltpu.get_barrier_semaphore()

    def here(zl, to_core, to_local):
        pl.semaphore_signal(
            barrier, inc=1, device_id=(2 * zl + to_core, to_local), device_id_type=MESH
        )

    for h in range(2):
        for step in range(1, 4):
            here(z_low, 1, along_first(h, step)[1])
    for step in range(1, 4):
        here(ahead(z_low, step), 0, local)
    here(z_low, 0, me_y * 8 + me_x * 2 + 1 - me_z)

    @pl.when(core == 0)
    def _():
        here(z_low, 1, local)

    def tell_other_core():
        pl.semaphore_signal(
            told, inc=1, device_id=(2 * z_low + 1 - core, local), device_id_type=MESH
        )

    def tile_of(own, dy, dx):
        return ahead(me_y, dy) * 8 + ahead(me_x, dx) * 2 + place_z(own)

    def slot_of(own, dy, dx):
        return 16 * own + 4 * NEAR_LAST.index(dy) + NEAR_LAST.index(dx)

    def start_loads(group):
        first, last = LOADS[group]
        for slot in range(first, last):
            own, dy, dx = slot // 16, NEAR_LAST[slot // 4 % 4], NEAR_LAST[slot % 4]
            t = tile_of(own, dy, dx)
            pltpu.make_async_copy(x_hbm.at[:, t], x_in.at[slot], in_sem.at[0, group]).start()
            pltpu.make_async_copy(
                signs_hbm.at[:, t], signs_in.at[slot], in_sem.at[1, group]
            ).start()

    def wait_loads(group):
        first, last = LOADS[group]
        for n, buffer in enumerate((x_in, signs_in)):
            whole = buffer.at[pl.ds(first, last - first)]
            pltpu.make_async_copy(whole, whole, in_sem.at[n, group]).wait()

    start_loads(0)
    own_copy = pltpu.make_async_copy(signs_hbm.at[node, local], own_signs, in_sem.at[0, len(LOADS)])
    own_copy.start()

    i = lax.broadcasted_iota(jnp.int32, (ROT, ROT), 0)
    j = lax.broadcasted_iota(jnp.int32, (ROT, ROT), 1)
    odd = lax.population_count(i & j) & 1
    matrix[...] = (1 - 2 * odd).astype(jnp.float32).astype(jnp.bfloat16)

    def rows_of(p):
        return pl.ds(PARTS[p][1], PARTS[p][2])

    def send_a(p, h, c, step):
        own = PARTS[p][0]
        return pltpu.make_async_remote_copy(
            src_ref=coded.at[h, own, c, ahead(first_of[h], step), rows_of(p)],
            dst_ref=got_a.at[h, own, c, step - 1, rows_of(p)],
            send_sem=a_send,
            recv_sem=a_recv.at[h, p, c],
            device_id=along_first(h, step),
            device_id_type=MESH,
        )

    def send_b(p, h, step):
        own = PARTS[p][0]
        return pltpu.make_async_remote_copy(
            src_ref=part.at[h, own, ahead(second_of[h], step), rows_of(p)],
            dst_ref=got_b.at[h, own, step - 1, rows_of(p)],
            send_sem=b_send,
            recv_sem=b_recv.at[h, p],
            device_id=along_second(h, step),
            device_id_type=MESH,
        )

    def send_c(p, h):
        return pltpu.make_async_remote_copy(
            src_ref=pair.at[h, rows_of(p)],
            dst_ref=got_c.at[h, rows_of(p)],
            send_sem=c_send,
            recv_sem=c_recv.at[h, p],
            device_id=device(me_y, me_x, 1 - me_z),
            device_id_type=MESH,
        )

    def send_n(h, k):
        z = z_low
        if k & 4:
            z = lax.rem(z + 2, 4)
        if k & 2:
            z = z + 1 - 2 * lax.rem(z, 2)
        to = 2 * z + (1 - core if k & 1 else core)
        return pltpu.make_async_remote_copy(
            src_ref=recoded.at[to, h],
            dst_ref=got_n.at[h, k - 1],
            send_sem=n_send,
            recv_sem=n_recv.at[h],
            device_id=(to, local),
            device_id_type=MESH,
        )

    def rotate(own, dy, steps):
        for k, dx in enumerate(steps):
            t = slot_of(own, dy, dx)
            for g in range(8):
                for q in range(4):
                    v = x_in[t, g, :, pl.ds(q * 1024, 1024)].astype(jnp.float32).reshape(8, 128)
                    s = signs_in[t, g, pl.ds(q * 8, 8), :]
                    rows[k, pl.ds(g * 32 + q * 8, 8), :] = jnp.where(s == 0, v, -v)
        for k, dx in enumerate(steps):
            blocks = jnp.concatenate(
                [
                    rows[k, pl.ds(0, 128, 2), :].astype(jnp.bfloat16),
                    rows[k, pl.ds(1, 128, 2), :].astype(jnp.bfloat16),
                ],
                axis=1,
            )
            rotated = lax.dot_general(
                matrix[...],
                blocks,
                (((1,), (1,)), ((), ())),
                preferred_element_type=jnp.float32,
            )
            y, x = ahead(me_y, dy), ahead(me_x, dx)
            coded[0, own, y, x] = encode(rotated[:QGROUP]).astype(jnp.bfloat16)
            coded[1, own, x, y] = encode(rotated[QGROUP:]).astype(jnp.bfloat16)

    def send_tiles(dy, steps):
        for dx in steps:
            if dx:
                send_a(0, 0, ahead(me_y, dy), dx).start()
            if dy:
                send_a(0, 1, ahead(me_x, dx), dy).start()

    def send_chunk(p, step):
        for to in NEAR_LAST[:3]:
            for h in range(2):
                send_a(p, h, ahead(second_of[h], step), to).start()

    def wait_for(buffer, sem):
        pltpu.make_async_copy(buffer, buffer, sem).wait()

    def send_near(side, *steps):
        @pl.when(me_z == side)
        def _():
            for step in steps:
                send_chunk(2, step)

    def reduce_first(p, step):
        own, rows = PARTS[p][0], rows_of(p)
        for h in range(2):
            c = ahead(second_of[h], step)
            wait_for(got_a.at[h, own, c, pl.ds(0, 3), rows], a_recv.at[h, p, c])
            total = coded[h, own, c, first_of[h], rows].astype(jnp.float32)
            for k in range(3):
                total += got_a[h, own, c, k, rows].astype(jnp.float32)
            part[h, own, c, rows] = total
            if step:
                send_b(p, h, step).start()

    def reduce_second(p, h):
        own, rows = PARTS[p][0], rows_of(p)
        wait_for(got_b.at[h, own, pl.ds(0, 3), rows], b_recv.at[h, p])
        total = part[h, own, second_of[h], rows]
        for k in range(3):
            total += got_b[h, own, k, rows]
        return total

    def exchange_z(p):
        for h in range(2):
            pair[h, rows_of(p)] = reduce_second(p, h)
            send_c(p, h).start()

    first_row, *other_rows = NEAR_LAST
    wait_loads(0)
    rotate(0, first_row, NEAR_LAST[:2])
    for group in range(1, len(LOADS)):
        start_loads(group)

    @pl.when(core == 1)
    def _():
        pl.semaphore_wait(barrier, 13)
        tell_other_core()

    @pl.when(core == 0)
    def _():
        pl.semaphore_wait(told, 1)

    send_tiles(first_row, NEAR_LAST[:2])
    wait_loads(1)
    rotate(0, first_row, NEAR_LAST[2:])
    send_tiles(first_row, NEAR_LAST[2:])
    for n, dy in enumerate(other_rows):
        wait_loads(2 + n)
        rotate(0, dy, NEAR_LAST)
        send_tiles(dy, NEAR_LAST)
    for step in NEAR_LAST:
        send_chunk(1, step)
    wait_loads(5)
    for dy in NEAR_LAST:
        rotate(1, dy, NEAR_LAST)
    for step in NEAR_LAST:
        reduce_first(0, step)
    send_near(0, 2)
    for step in NEAR_LAST:
        reduce_first(1, step)
    send_near(0, 1)

    @pl.when(core == 0)
    def _():
        pl.semaphore_wait(barrier, 8)
        tell_other_core()

    @pl.when(core == 1)
    def _():
        pl.semaphore_wait(told, 1)

    send_near(0, 3, 0)
    exchange_z(0)
    exchange_z(1)
    send_near(1, 2, 1, 3, 0)
    for step in NEAR_LAST:
        reduce_first(2, step)
    for h in range(2):
        first = reduce_second(2, h)
        wait_for(got_c.at[h, rows_of(0)], c_recv.at[h, 0])
        wait_for(got_c.at[h, rows_of(1)], c_recv.at[h, 1])
        decoded = encode(first + got_c[h])
        recoded[:, h] = decoded.T.astype(jnp.bfloat16).reshape(8, 16, QGROUP)
        for k in FAR_FIRST:
            send_n(h, k).start()
    own_copy.wait()
    wait_for(got_a, a_send)
    wait_for(got_b, b_send)
    wait_for(got_c, c_send)
    second = [recoded[node, h].astype(jnp.float32) for h in range(2)]
    for h in range(2):
        wait_for(got_n.at[h], n_recv.at[h])
        for k in reversed(FAR_FIRST):
            second[h] += got_n[h, k - 1].astype(jnp.float32)

    lane = lax.broadcasted_iota(jnp.int32, (16, 32), 1)
    block = lax.broadcasted_iota(jnp.int32, (16, 32), 0)
    widest = jnp.zeros((1, 32), jnp.float32)
    for h in range(2):
        most = jnp.max(jnp.abs(second[h]), axis=1, keepdims=True) * (1.0 / 16.0)
        widest += jnp.sum(jnp.where(lane == 2 * block + h, most, 0.0), axis=0, keepdims=True)
    max_ref[...] = widest

    whole = jnp.concatenate(second, axis=1)
    high = whole.astype(jnp.bfloat16)
    rest = whole - high.astype(jnp.float32)
    middle = rest.astype(jnp.bfloat16)
    low = (rest - middle.astype(jnp.float32)).astype(jnp.bfloat16)
    pieces = jnp.concatenate([high, middle, low], axis=0)
    back = jnp.dot(pieces, matrix[...], preferred_element_type=jnp.float32)
    back = ((back[32:48] + back[16:32]) + back[0:16]) * (1.0 / ROT)
    for h in range(2):
        s = own_signs[pl.ds(h, 16, 2), :]
        half = back[:, h * QGROUP : (h + 1) * QGROUP]
        out_ref[pl.ds(h, 16, 2), :] = jnp.where(s == 0, half, -half)

    wait_for(got_n, n_send)


def finish(turned_ref, most_ref, out_ref, max_ref, sem):
    copies = (
        pltpu.make_async_copy(turned_ref, out_ref, sem.at[0]),
        pltpu.make_async_copy(most_ref, max_ref, sem.at[1]),
    )
    for copy in copies:
        copy.start()
    for copy in copies:
        copy.wait()


def shards(partials, signs):
    dma = pltpu.SemaphoreType.DMA
    turned, most = pl.pallas_call(
        kernel,
        out_shape=(pltpu.VMEM((32, QGROUP), jnp.float32), pltpu.VMEM((1, 32), jnp.float32)),
        in_specs=[pl.BlockSpec(memory_space=pl.ANY)] * 2,
        out_specs=(
            pl.BlockSpec(memory_space=pltpu.VMEM),
            pl.BlockSpec(memory_space=pltpu.VMEM),
        ),
        scratch_shapes=[
            pltpu.VMEM((32, 8, 1, 4096), jnp.bfloat16),
            pltpu.VMEM((32, 8, 32, QGROUP), jnp.int32),
            pltpu.VMEM((32, QGROUP), jnp.int32),
            pltpu.VMEM((ROT, ROT), jnp.bfloat16),
            pltpu.VMEM((4, ROT, QGROUP), jnp.float32),
            pltpu.VMEM((2, 2, 4, 4, QGROUP, QGROUP), jnp.bfloat16),
            pltpu.VMEM((2, 2, 4, 3, QGROUP, QGROUP), jnp.bfloat16),
            pltpu.VMEM((2, 2, 4, QGROUP, QGROUP), jnp.float32),
            pltpu.VMEM((2, 2, 3, QGROUP, QGROUP), jnp.float32),
            pltpu.VMEM((2, QGROUP, QGROUP), jnp.float32),
            pltpu.VMEM((2, QGROUP, QGROUP), jnp.float32),
            pltpu.VMEM((8, 2, 16, QGROUP), jnp.bfloat16),
            pltpu.VMEM((2, 7, 16, QGROUP), jnp.bfloat16),
            pltpu.SemaphoreType.REGULAR,
            dma((2, len(LOADS) + 1)),
            dma,
            dma((2, 3, 4)),
            dma,
            dma((2, 3)),
            dma,
            dma((2, 2)),
            dma,
            dma((2,)),
        ],
        compiler_params=pltpu.CompilerParams(collective_id=0, has_side_effects=True),
    )(partials.reshape(8, 32, 1, 4096), signs.reshape(8, 32, 32, QGROUP))
    out, widest = pl.pallas_call(
        finish,
        out_shape=(
            jax.ShapeDtypeStruct((32, QGROUP), jnp.float32),
            jax.ShapeDtypeStruct((1, 32), jnp.float32),
        ),
        in_specs=[pl.BlockSpec(memory_space=pltpu.VMEM)] * 2,
        out_specs=[pl.BlockSpec(memory_space=pl.ANY)] * 2,
        scratch_shapes=[dma((2,))],
    )(
        pltpu.with_memory_space_constraint(turned, pltpu.VMEM),
        pltpu.with_memory_space_constraint(most, pltpu.VMEM),
    )
    return out.reshape(-1), widest.reshape(-1)


def solution(mesh):
    in_specs = (P("node", "local", None), P())
    out_specs = (P(("node", "local")), P(("node", "local")))
    return jax.shard_map(shards, mesh=mesh, in_specs=in_specs, out_specs=out_specs, check_vma=False)
```
